128 devices in a mesh: box: 4 (over z), leaf: 32 (over y, x, core).
Axes of the slice: x: 4, y: 4, z: 4, core: 2. Of those that a mesh axis runs over, the one named last changes fastest.
Arguments:
- probes: bfloat16 [64, 524288], P(None, ('box', 'leaf')), may hold values from -6 to 6
- near_index: int32 [8192, 8], P(('box', 'leaf')), may hold values from 0 to 8191, as said below
- far_index: int32 [8192, 8], P(('box', 'leaf')), may hold values from 0 to 8191, as said below
- inner_near: bfloat16 [8, 64, 524288], P(None, None, ('box', 'leaf')), may hold values from -0.25 to 0.25
- inner_basis: bfloat16 [64, 524288], P(None, ('box', 'leaf')), may hold values from -0.75 to 0.75
- inner_far: bfloat16 [8, 64, 524288], P(None, None, ('box', 'leaf')), may hold values from -0.25 to 0.25
- inner_transfer: bfloat16 [64, 524288], P(None, ('box', 'leaf')), may hold values from -0.09375 to 0.09375
- inner_tree: bfloat16 [2, 2, 64, 8192], P(None, None, None, ('box', 'leaf')), as said below
- inner_links: bfloat16 [3, 3, 64, 8192], P(None, None, None, ('box', 'leaf')), as said below
- outer_near: bfloat16 [8, 64, 524288], P(None, None, ('box', 'leaf')), may hold values from -0.25 to 0.25
- outer_basis: bfloat16 [64, 524288], P(None, ('box', 'leaf')), may hold values from -0.75 to 0.75
- outer_far: bfloat16 [8, 64, 524288], P(None, None, ('box', 'leaf')), may hold values from -0.25 to 0.25
- outer_transfer: bfloat16 [64, 524288], P(None, ('box', 'leaf')), may hold values from -0.09375 to 0.09375
- outer_tree: bfloat16 [2, 2, 64, 8192], P(None, None, None, ('box', 'leaf')), as said below
- outer_links: bfloat16 [3, 3, 64, 8192], P(None, None, None, ('box', 'leaf')), as said below
Outputs:
- pair_basis: float32 [64, 524288], P(None, ('box', 'leaf'))
- group_basis: float32 [64, 262144], P(None, ('box', 'leaf'))
The draws below stay inside these ranges and needn't reach their ends.
Inputs may be any that keep to these rules, and one draw needn't show every extreme that they name: near_index[i, 0] = i; every other entry differs from i by 1 to 64. `far_index`: every entry differs from i by 1 to 64. inner_tree[c, j] holds equal blocks on all nodes of one cluster of level c + 1. inner_links[c, s] holds equal blocks on all nodes of one cluster of level c. outer_tree[c, j] holds equal blocks on all nodes of one cluster of level c + 1. outer_links[c, s] holds equal blocks on all nodes of one cluster of level c.
All inputs are finite; a program needn't handle non-finite values.
Results may differ from the reference program's by a relative error of at most 0.0078.
Values may be sent and summed in bfloat16 or wider, within the bound.
No kernel may reach another device: no remote copies, remote signals or barrier semaphores. Data moves between devices by JAX's collectives and lax.ppermute only.
A program may use at most 192 MiB of HBM per device.

```python
import jax
import jax.numpy as jnp
from jax import lax

LEAF = 64
RANK = 64
PROBES = 64
NEAR = 8
FAR = 8
CLEVELS = 3
LPD = 64
NODES = 128
NLEAVES = 8192
ROWS = 524288
GROUP_PAIRS = 1024
N_BOX = 4


def neighbour_lists(key):
    options = 2 * LPD
    scores = jax.random.randint(jax.random.fold_in(key, 7), (NLEAVES, options), 0, 1 << 20)
    scores = scores * options + jnp.arange(options, dtype=jnp.int32)[None, :]
    picked = jnp.argsort(scores, axis=1)[:, :NEAR - 1 + FAR].astype(jnp.int32)
    offsets = jnp.where(picked < LPD, picked - LPD, picked - LPD + 1)
    leaves = jnp.arange(NLEAVES, dtype=jnp.int32)[:, None]
    target = leaves + offsets
    target = jnp.where((target < 0) | (target >= NLEAVES), leaves - offsets, target)
    near = jnp.concatenate([leaves, target[:, :NEAR - 1]], axis=1)
    return (near.astype(jnp.int32), target[:, NEAR - 1:].astype(jnp.int32))


def random_blocks(key, shape):
    return jax.random.normal(key, shape, jnp.float32)


def tree_draw(key, salt):
    levels = []
    for height in range(CLEVELS - 1):
        span = 2 ** (height + 1)
        blocks = random_blocks(jax.random.fold_in(key, salt * 100 + height), (2, RANK, NODES // span, RANK))
        blocks = blocks * (2.0 * RANK) ** (-0.5)
        levels.append(jnp.repeat(blocks, span, axis=2).reshape(2, RANK, NODES * RANK))
    return jnp.stack(levels).astype(jnp.bfloat16)


def links_draw(key, salt):
    levels = []
    for height in range(CLEVELS):
        span = 2 ** height
        blocks = random_blocks(jax.random.fold_in(key, salt * 100 + height), (3, RANK, NODES // span, RANK))
        blocks = blocks * (3.0 * RANK) ** (-0.5)
        levels.append(jnp.repeat(blocks, span, axis=2).reshape(3, RANK, NODES * RANK))
    return jnp.stack(levels).astype(jnp.bfloat16)


def draw_near_index(key, part):
    return neighbour_lists(key)[0]


def draw_far_index(key, part):
    return neighbour_lists(key)[1]


def draw_inner_tree(key, part):
    return tree_draw(key, 11)


def draw_inner_links(key, part):
    return links_draw(key, 13)


def draw_outer_tree(key, part):
    return tree_draw(key, 17)


def draw_outer_links(key, part):
    return links_draw(key, 19)


def block_levels(stream_key, dims, split, low, largest):
    level = 1.0
    for axis_at, parts in split:
        steps = jax.random.uniform(jax.random.fold_in(jax.random.fold_in(stream_key, 6), axis_at), (parts,), jnp.float32, low / len(split), largest / len(split))
        level = level * jnp.repeat(jnp.exp(steps), dims[axis_at] // parts).reshape((-1,) + (1,) * (len(dims) - 1 - axis_at))
    return level


def scatter_about(own_key, shape, spread, most, pieces=(), kind=jnp.bfloat16):
    factor_of = block_levels(own_key, shape, pieces, -0.22, 0.18) if pieces else 1.0
    array = jax.random.normal(own_key, shape, jnp.float32) * spread * factor_of
    return jnp.minimum(jnp.maximum(array, -most), most).astype(kind)


def setup_inputs(seed: int = 0) -> dict:
    key_of = jax.random.split(jax.random.key(seed), 16)
    probes = scatter_about(key_of[0], (PROBES, ROWS), 1.0, 6.0, ((1, 128),))
    near_index = draw_near_index(jax.random.fold_in(key_of[15], 71), 0)
    far_index = draw_far_index(jax.random.fold_in(key_of[15], 71), 0)
    inner_near = scatter_about(key_of[3], (NEAR, LEAF, ROWS), (NEAR * LEAF) ** -0.5, 0.25, ((2, 128),))
    inner_basis = scatter_about(key_of[4], (RANK, ROWS), LEAF ** -0.5, 0.75, ((1, 128),))
    inner_far = scatter_about(key_of[5], (FAR, RANK, NLEAVES * RANK), (FAR * RANK) ** -0.5, 0.25, ((2, 128),))
    inner_transfer = scatter_about(key_of[6], (RANK, NLEAVES * RANK), (LPD * RANK) ** -0.5, 0.09375, ((1, 128),))
    inner_tree = draw_inner_tree(jax.random.fold_in(key_of[15], 71), 0)
    inner_links = draw_inner_links(jax.random.fold_in(key_of[15], 71), 0)
    outer_near = scatter_about(key_of[9], (NEAR, LEAF, ROWS), (NEAR * LEAF) ** -0.5, 0.25, ((2, 128),))
    outer_basis = scatter_about(key_of[10], (RANK, ROWS), LEAF ** -0.5, 0.75, ((1, 128),))
    outer_far = scatter_about(key_of[11], (FAR, RANK, NLEAVES * RANK), (FAR * RANK) ** -0.5, 0.25, ((2, 128),))
    outer_transfer = scatter_about(key_of[12], (RANK, NLEAVES * RANK), (LPD * RANK) ** -0.5, 0.09375, ((1, 128),))
    outer_tree = draw_outer_tree(jax.random.fold_in(key_of[15], 71), 0)
    outer_links = draw_outer_links(jax.random.fold_in(key_of[15], 71), 0)
    return dict(probes=probes, near_index=near_index, far_index=far_index, inner_near=inner_near, inner_basis=inner_basis, inner_far=inner_far, inner_transfer=inner_transfer, inner_tree=inner_tree, inner_links=inner_links, outer_near=outer_near, outer_basis=outer_basis, outer_far=outer_far, outer_transfer=outer_transfer, outer_tree=outer_tree, outer_links=outer_links)


highest = lax.Precision.HIGHEST

def settle(values):
    return lax.optimization_barrier(values.astype(jnp.bfloat16)).astype(jnp.float32)

def coarse_reference(node_coords, tree, links):
    heights = [node_coords]
    for height in range(CLEVELS - 1):
        span = 2 ** (height + 1)
        blocks = tree[height].reshape(2, RANK, NODES, RANK)[:, :, ::span, :].astype(jnp.float32)
        current = heights[height]
        parent = jnp.einsum('tpk,ktl->tpl', current[0::2], blocks[0], precision=highest)
        parent = parent + jnp.einsum('tpk,ktl->tpl', current[1::2], blocks[1], precision=highest)
        heights.append(parent)
    coupled = []
    for height in range(CLEVELS):
        current = heights[height]
        count = current.shape[0]
        blocks = links[height].reshape(3, RANK, NODES, RANK)[:, :, ::2 ** height, :].astype(jnp.float32)
        padded = jnp.pad(current, ((4, 4), (0, 0), (0, 0)))
        place = jnp.arange(count, dtype=jnp.int32)
        base = 2 * (place // 2) + 4
        left_low = padded[base - 2]
        left_high = padded[base - 1]
        right_low = padded[base + 2]
        right_high = padded[base + 3]
        middle = jnp.where((place % 2 == 0)[:, None, None], right_low, left_high)
        summed = jnp.einsum('tpk,ktl->tpl', left_low, blocks[0], precision=highest)
        summed = summed + jnp.einsum('tpk,ktl->tpl', middle, blocks[1], precision=highest)
        summed = summed + jnp.einsum('tpk,ktl->tpl', right_high, blocks[2], precision=highest)
        coupled.append(summed)
    descent = coupled[CLEVELS - 1]
    for height in range(CLEVELS - 2, -1, -1):
        span = 2 ** (height + 1)
        blocks = tree[height].reshape(2, RANK, NODES, RANK)[:, :, ::span, :].astype(jnp.float32)
        owned = jnp.transpose(blocks, (2, 0, 1, 3)).reshape(-1, RANK, RANK)
        widened = jnp.repeat(descent, 2, axis=0)
        descent = coupled[height] + jnp.einsum('tpl,tkl->tpk', widened, owned, precision=highest)
    return descent

def apply_matrix(samples, near_index, far_index, near, basis, far, transfer, tree, links):
    probe = samples.shape[0]
    rows3 = samples.reshape(probe, NLEAVES, LEAF)
    basis3 = basis.reshape(RANK, NLEAVES, LEAF)
    transfer3 = transfer.reshape(RANK, NLEAVES, RANK)
    coords = jnp.einsum('pim,kim->pik', rows3.astype(jnp.float32), basis3.astype(jnp.float32), precision=highest)
    coords = lax.optimization_barrier(coords.astype(jnp.bfloat16))
    node_coords = jnp.einsum('pqik,kqil->qpl', coords.reshape(probe, NODES, LPD, RANK).astype(jnp.float32), transfer3.reshape(RANK, NODES, LPD, RANK).astype(jnp.float32), precision=highest)
    descent = settle(coarse_reference(node_coords, tree, links))

    def node_block(node):
        start = node * LPD
        near_rows = jnp.take(rows3, lax.dynamic_slice_in_dim(near_index, start, LPD, 0), axis=1).astype(jnp.float32)
        near_local = lax.dynamic_slice_in_dim(near, start * LEAF, LPD * LEAF, 2).reshape(NEAR, LEAF, LPD, LEAF).astype(jnp.float32)
        near_part = jnp.einsum('pisa,saib->pib', near_rows, near_local, precision=highest)
        far_rows = jnp.take(coords, lax.dynamic_slice_in_dim(far_index, start, LPD, 0), axis=1).astype(jnp.float32)
        far_local = lax.dynamic_slice_in_dim(far, start * RANK, LPD * RANK, 2).reshape(FAR, RANK, LPD, RANK).astype(jnp.float32)
        far_part = jnp.einsum('pisk,skil->pil', far_rows, far_local, precision=highest)
        local_transfer = lax.dynamic_slice_in_dim(transfer3, start, LPD, 1).astype(jnp.float32)
        down_part = jnp.einsum('pl,kil->pik', descent[node], local_transfer, precision=highest)
        leaf_coeffs = settle(far_part + down_part)
        local_basis = lax.dynamic_slice_in_dim(basis3, start, LPD, 1).astype(jnp.float32)
        return near_part + jnp.einsum('pik,kim->pim', leaf_coeffs, local_basis, precision=highest)
    blocks = lax.map(node_block, jnp.arange(NODES, dtype=jnp.int32))
    return jnp.transpose(blocks, (1, 0, 2, 3)).reshape(probe, NLEAVES * LEAF)

def reference(probes, near_index, far_index, inner_near, inner_basis, inner_far, inner_transfer, inner_tree, inner_links, outer_near, outer_basis, outer_far, outer_transfer, outer_tree, outer_links):
    middle = apply_matrix(probes, near_index, far_index, inner_near, inner_basis, inner_far, inner_transfer, inner_tree, inner_links)
    middle = lax.optimization_barrier(middle.astype(jnp.bfloat16))
    samples = apply_matrix(middle, near_index, far_index, outer_near, outer_basis, outer_far, outer_transfer, outer_tree, outer_links)
    probe = samples.shape[0]
    pairs = NLEAVES // 2
    blocks = jnp.transpose(samples.reshape(probe, pairs, 2 * LEAF), (1, 0, 2))
    gram = jnp.einsum('rpm,rqm->rpq', blocks, blocks, precision=highest) / (2 * LEAF)
    lower = jnp.linalg.cholesky(gram)
    pair_q = jax.scipy.linalg.solve_triangular(lower, blocks, lower=True)
    grouped = lower.reshape(N_BOX, GROUP_PAIRS, probe, probe)
    group_gram = jnp.einsum('grab,grcb->gac', grouped, grouped, precision=highest) / GROUP_PAIRS
    group_lower = jnp.linalg.cholesky(group_gram)
    group_q = jax.scipy.linalg.solve_triangular(jnp.repeat(group_lower, GROUP_PAIRS, axis=0), lower, lower=True)
    pair_basis = jnp.transpose(pair_q, (1, 0, 2)).reshape(probe, NLEAVES * LEAF)
    group_basis = jnp.transpose(group_q, (1, 0, 2)).reshape(probe, pairs * probe)
    return (pair_basis, group_basis)
```

```python
import jax
import jax.numpy as jnp
from jax import lax
from jax.experimental import pallas as pl
from jax.experimental.pallas import tpu as pltpu
from jax.sharding import PartitionSpec as P

AXES = ("box", "leaf")
LEAF = 64
TILE = 128
STEPS = 8
bf16 = jnp.bfloat16
f32 = jnp.float32
highest = lax.Precision.HIGHEST

NN = (((1,), (0,)), ((), ()))
NT = (((1,), (1,)), ((), ()))


def dot(a, b, dims=NN, precision=None):
    return lax.dot_general(a, b, dims, precision=precision, preferred_element_type=f32)


def low_half(shape):
    return lax.broadcasted_iota(jnp.int32, shape, len(shape) - 1) < LEAF


def two_blocks(tile):
    low = low_half(tile.shape)
    zero = jnp.zeros_like(tile)
    return jnp.concatenate([jnp.where(low, tile, zero), jnp.where(low, zero, tile)], axis=0)


def swap_halves(tile):
    return jnp.concatenate([tile[:, LEAF:], tile[:, :LEAF]], axis=1)


def twice(block):
    return jnp.concatenate([block, block], axis=1)


def lanes(t):
    return pl.ds(pl.multiple_of(t * TILE, TILE), TILE)


def coarse_payload(sums, tree_ref, scal_ref, pay_ref):
    folded = sums + swap_halves(sums)
    pay_ref[0] = folded.astype(bf16)
    up = dot(folded[:, :LEAF].astype(bf16), tree_ref[0, scal_ref[0]])
    pay_ref[1] = twice(up).astype(bf16)
    up = dot(up.astype(bf16), tree_ref[1, scal_ref[1]])
    pay_ref[2] = twice(up).astype(bf16)


def coords_kernel(scal_ref, rows_ref, basis_ref, transfer_ref, tree_ref, coords_ref, pay_ref):
    def step(g, sums):
        for u in range(4):
            at = lanes(g * 4 + u)
            coords = dot(rows_ref[:, at], two_blocks(basis_ref[:, at]), NT).astype(bf16)
            coords_ref[:, at] = coords
            sums = sums + dot(coords, two_blocks(transfer_ref[:, at]))
        return sums

    count = rows_ref.shape[1] // TILE
    sums = lax.fori_loop(0, count // 4, step, jnp.zeros((LEAF, TILE), f32))
    coarse_payload(sums, tree_ref, scal_ref, pay_ref)


def fill_store(store_ref, sources):
    tiles = sources[0].shape[1] // TILE
    half = store_ref.shape[0] // 2
    for n, source in enumerate(sources):

        def step(g, carry, n=n, source=source):
            for u in range(4):
                t = g * 4 + u
                tile = source[:, lanes(t)]
                store_ref[n * tiles + t] = tile
                store_ref[half + n * tiles + t] = swap_halves(tile)
            return carry

        lax.fori_loop(0, tiles // 4, step, 0)


def gathered(store_ref, index_ref, pair, low):
    rows = []
    for h in range(2):
        base = (2 * pair + h) * 8
        cols = []
        for k in range(4):
            first = store_ref[index_ref[base + 2 * k]]
            second = store_ref[index_ref[base + 2 * k + 1]]
            cols.append(jnp.where(low, first, second))
        rows.append(jnp.concatenate(cols, axis=1))
    return jnp.concatenate(rows, axis=0)


def descend(scal_ref, mine_ref, other_ref, first_ref, second_ref, tree_ref, links_ref):
    b0, b1, b2 = scal_ref[0], scal_ref[1], scal_ref[2]
    odd, has_left, has_right = scal_ref[3], scal_ref[4], scal_ref[5]

    def low_group(n):
        return jnp.where(b2 == 0, mine_ref[n], other_ref[n])

    def high_group(n):
        return jnp.where(b2 == 0, other_ref[n], mine_ref[n])

    def left(n):
        tile = jnp.where(odd == 1, first_ref[n], second_ref[n])
        return jnp.where(has_left == 1, tile, jnp.zeros_like(tile))

    def right(n):
        tile = jnp.where(odd == 1, second_ref[n], first_ref[n])
        return jnp.where(has_right == 1, tile, jnp.zeros_like(tile))

    def pick(j, options):
        tile = options[-1]
        for n in range(len(options) - 2, -1, -1):
            tile = jnp.where(j == n, options[n], tile)
        return tile

    ext0 = [left(2), low_group(0), low_group(1), high_group(0), high_group(1), right(2)]
    ext1 = [left(1), low_group(2), high_group(2), right(1)]
    j0, j1 = b2 * 2 + b1, b2
    around = [
        (pick(j0, ext0[:4]), pick(j0, ext0[2:])),
        (pick(j1, ext1[:2]), pick(j1, ext1[2:])),
        (left(0), right(0)),
    ]
    coupled = []
    for c, parity in enumerate((b0, b1, b2)):
        mid = links_ref[c, 1]
        none = jnp.zeros_like(mid)
        lo = jnp.concatenate([links_ref[c, 0], jnp.where(parity == 1, mid, none)], axis=0)
        hi = jnp.concatenate([jnp.where(parity == 0, mid, none), links_ref[c, 2]], axis=0)
        coupled.append(dot(around[c][0], lo) + dot(around[c][1], hi))
    h = coupled[1] + dot(coupled[2].astype(bf16), tree_ref[1, b1], NT)
    h = coupled[0] + dot(h.astype(bf16), tree_ref[0, b0], NT)
    return twice(h).astype(bf16)


def apply_tile(u, pair, low, refs):
    near_index, far_index, near_ref, far_ref, basis_ref, transfer_ref, rows_store, coords_store, descent = refs
    at = slice(u * TILE, (u + 1) * TILE)
    near = near_ref[:, :, at].reshape(8 * LEAF, TILE)
    far = far_ref[:, :, at].reshape(8 * LEAF, TILE)
    low32 = low_half((LEAF, TILE))
    near_all = dot(gathered(rows_store, near_index, pair, low), near)
    far_all = dot(gathered(coords_store, far_index, pair, low), far)
    near_part = jnp.where(low32, near_all[:LEAF], near_all[LEAF:])
    far_part = jnp.where(low32, far_all[:LEAF], far_all[LEAF:])
    down = dot(descent, two_blocks(transfer_ref[:, at]), NT)
    coeffs = (far_part + down).astype(bf16)
    return near_part + dot(coeffs, two_blocks(basis_ref[:, at]))


def prepare(step, scal_ref, rows_refs, coords_refs, coarse_refs, tree_ref, links_ref, rows_store, coords_store, descent_ref):
    @pl.when(step == 0)
    def _():
        fill_store(rows_store, rows_refs)
        fill_store(coords_store, coords_refs)
        descent_ref[...] = descend(scal_ref, *coarse_refs, tree_ref, links_ref)


def inner_kernel(
    scal_ref, near_index, far_index,
    rows_b, rows_own, rows_a, coords_b, coords_own, coords_a,
    mine_ref, other_ref, first_ref, second_ref, tree_ref, links_ref, next_tree_ref,
    near_ref, far_ref, basis_ref, transfer_ref, next_basis_ref, next_transfer_ref,
    middle_ref, next_coords_ref, pay_ref,
    rows_store, coords_store, descent_ref, sums_ref,
):
    step = pl.program_id(0)
    prepare(
        step, scal_ref, (rows_b, rows_own, rows_a), (coords_b, coords_own, coords_a),
        (mine_ref, other_ref, first_ref, second_ref), tree_ref, links_ref,
        rows_store, coords_store, descent_ref,
    )

    @pl.when(step == 0)
    def _():
        sums_ref[...] = jnp.zeros_like(sums_ref)

    low = low_half((LEAF, TILE))
    refs = (near_index, far_index, near_ref, far_ref, basis_ref, transfer_ref, rows_store, coords_store, descent_ref[...])
    per = near_ref.shape[2] // TILE
    sums = sums_ref[...]
    for u in range(per):
        at = slice(u * TILE, (u + 1) * TILE)
        middle = apply_tile(u, step * per + u, low, refs).astype(bf16)
        middle_ref[:, at] = middle
        coords = dot(middle, two_blocks(next_basis_ref[:, at]), NT).astype(bf16)
        next_coords_ref[:, at] = coords
        sums = sums + dot(coords, two_blocks(next_transfer_ref[:, at]))
    sums_ref[...] = sums

    @pl.when(step == pl.num_programs(0) - 1)
    def _():
        coarse_payload(sums, next_tree_ref, scal_ref, pay_ref)


def outer_kernel(
    scal_ref, near_index, far_index,
    rows_b, rows_own, rows_a, coords_b, coords_own, coords_a,
    mine_ref, other_ref, first_ref, second_ref, tree_ref, links_ref,
    near_ref, far_ref, basis_ref, transfer_ref,
    samples_ref, gram_ref,
    rows_store, coords_store, descent_ref,
):
    step = pl.program_id(0)
    prepare(
        step, scal_ref, (rows_b, rows_own, rows_a), (coords_b, coords_own, coords_a),
        (mine_ref, other_ref, first_ref, second_ref), tree_ref, links_ref,
        rows_store, coords_store, descent_ref,
    )

    @pl.when(step == 0)
    def _():
        gram_ref[...] = jnp.zeros_like(gram_ref)

    low = low_half((LEAF, TILE))
    refs = (near_index, far_index, near_ref, far_ref, basis_ref, transfer_ref, rows_store, coords_store, descent_ref[...])
    per = near_ref.shape[2] // TILE
    gram = gram_ref[...]
    for u in range(per):
        out = apply_tile(u, step * per + u, low, refs)
        samples_ref[:, u * TILE : (u + 1) * TILE] = out
        gram = gram + dot(out, out, NT, highest)
    gram_ref[...] = gram


def eliminate(work_ref):
    count = work_ref.shape[0]
    sub = lax.broadcasted_iota(jnp.int32, (count, 8, TILE), 1)
    for kb in range(LEAF // 8):
        panel = work_ref[:, kb * 8 : kb * 8 + 8, :]
        scaled = []
        for j in range(8):
            k = kb * 8 + j
            inv = lax.rsqrt(panel[:, j : j + 1, k : k + 1])
            row = panel[:, j : j + 1, :] * inv
            again = row * inv
            scaled.append(again)
            factor = jnp.where(sub > j, jnp.broadcast_to(panel[:, :, k : k + 1], sub.shape), 0.0)
            panel = jnp.where(sub == j, row, panel - factor * again)
        work_ref[:, kb * 8 : kb * 8 + 8, :] = panel
        for ib in range(kb + 1, LEAF // 8):
            rest = work_ref[:, ib * 8 : ib * 8 + 8, :]
            for j in range(8):
                k = kb * 8 + j
                rest = rest - rest[:, :, k : k + 1] * scaled[j]
            work_ref[:, ib * 8 : ib * 8 + 8, :] = rest


def identity_half():
    row = lax.broadcasted_iota(jnp.int32, (LEAF, LEAF), 0)
    col = lax.broadcasted_iota(jnp.int32, (LEAF, LEAF), 1)
    return jnp.where(row == col, 1.0, 0.0).astype(f32)


def pair_kernel(samples_ref, basis_ref, work_ref):
    count = samples_ref.shape[1] // TILE
    eye = identity_half()

    def gram_step(g, carry):
        for u in range(4):
            t = g * 4 + u
            tile = samples_ref[:, lanes(t)]
            work_ref[t] = jnp.concatenate([dot(tile, tile, NT, highest) / TILE, eye], axis=1)
        return carry

    lax.fori_loop(0, count // 4, gram_step, 0)
    eliminate(work_ref)

    def solve_step(g, carry):
        for u in range(4):
            t = g * 4 + u
            basis_ref[:, lanes(t)] = dot(work_ref[t][:, LEAF:], samples_ref[:, lanes(t)], NN, highest)
        return carry

    lax.fori_loop(0, count // 4, solve_step, 0)


def group_kernel(gram_ref, work_ref, out_ref, own_ref, *, scale):
    count = work_ref.shape[0]
    own_ref[0] = jnp.concatenate([gram_ref[...] / scale, identity_half()], axis=1)
    eliminate(own_ref)
    inverse = own_ref[0][:, LEAF:]
    row = lax.broadcasted_iota(jnp.int32, (LEAF, LEAF), 0)
    col = lax.broadcasted_iota(jnp.int32, (LEAF, LEAF), 1)
    upper = row <= col

    def step(g, carry):
        for u in range(4):
            t = g * 4 + u
            first = jnp.where(upper, work_ref[2 * t][:, :LEAF], 0.0)
            second = jnp.where(upper, work_ref[2 * t + 1][:, :LEAF], 0.0)
            out_ref[:, lanes(t)] = dot(inverse, jnp.concatenate([first, second], axis=0), NT, highest)
        return carry

    lax.fori_loop(0, count // 8, step, 0)


VMEM = pl.BlockSpec(memory_space=pltpu.VMEM)
SMEM = pl.BlockSpec(memory_space=pltpu.SMEM)


def params(mib):
    return pltpu.CompilerParams(vmem_limit_bytes=mib * 2**20)


def struct(shape, dtype):
    return jax.ShapeDtypeStruct(shape, dtype)


def swap(x, mask):
    count = lax.axis_size(AXES)
    return lax.ppermute(x, AXES, [(i, i ^ mask) for i in range(count)])


def neighbours(x, width, second):
    count = lax.axis_size(AXES)
    blocks = count // width
    route = []
    for b in range(blocks):
        forward = (b % 2 == 0) != second
        to = (b + 1 if forward else b - 1) % blocks
        route += [(b * width + m, to * width + m) for m in range(width)]
    return lax.ppermute(x, AXES, route)


def node_halo(x):
    count = lax.axis_size(AXES)
    route = [(i, (i - 1 if i % 2 == 0 else i + 1) % count) for i in range(count)]
    return lax.ppermute(x, AXES, route), swap(x, 1)


def leaf_table(index, node):
    leaves = index.shape[0]
    place = index - (node - 1) * leaves
    block = place // leaves
    block = jnp.where(node % 2 == 1, 2 - block, block)
    place = block * leaves + place % leaves
    slot = lax.broadcasted_iota(jnp.int32, index.shape, 1)
    return (((place + slot) % 2) * (3 * leaves // 2) + place // 2).reshape(-1)


def coarse_exchange(pay, node):
    low = low_half((LEAF, TILE))
    b0, b1, b2 = node % 2, node // 2 % 2, node // 4 % 2
    odd = node // 8 % 2

    def halves(bit, mine, other):
        return jnp.where(low == (bit == 0), mine, other)

    other = swap(pay, 1)
    z0 = halves(b0, pay[0], other[0])
    stage = jnp.stack([z0, pay[1] + other[1], pay[2] + other[2]])
    other = swap(stage, 2)
    first = jnp.where(b1 == 0, stage[0], other[0])
    second = jnp.where(b1 == 0, other[0], stage[0])
    mine = jnp.stack([first, second, halves(b1, stage[1], other[1]), stage[2] + other[2]])
    other = swap(mine, 6)
    top = halves(b2, mine[3], other[3])
    lo = jnp.where(b2 == 0, mine, other)
    hi = jnp.where(b2 == 0, other, mine)
    rightward = jnp.stack([top, hi[2], hi[1]])
    leftward = jnp.stack([top, lo[2], lo[0]])
    one = neighbours(jnp.where(odd == 0, rightward, leftward), 8, False)
    two = neighbours(jnp.where(odd == 0, leftward, rightward), 8, True)
    return mine, other, one, two


def local(
    probes,
    near_index,
    far_index,
    inner_near,
    inner_basis,
    inner_far,
    inner_transfer,
    inner_tree,
    inner_links,
    outer_near,
    outer_basis,
    outer_far,
    outer_transfer,
    outer_tree,
    outer_links,
):
    node = lax.axis_index(AXES)
    count = lax.axis_size(AXES)
    width = probes.shape[1]
    block = node // 8
    scal = jnp.stack(
        [
            node % 2,
            node // 2 % 2,
            node // 4 % 2,
            block % 2,
            (block > 0).astype(jnp.int32),
            (block < count // 8 - 1).astype(jnp.int32),
        ]
    ).astype(jnp.int32)
    near_table = leaf_table(near_index, node)
    far_table = leaf_table(far_index, node)

    rows_b, rows_a = node_halo(probes)
    coords, pay = pl.pallas_call(
        coords_kernel,
        in_specs=[SMEM, VMEM, VMEM, VMEM, VMEM],
        out_specs=(VMEM, VMEM),
        out_shape=(struct((LEAF, width), bf16), struct((3, LEAF, TILE), bf16)),
        compiler_params=params(16),
        name="coords",
    )(scal, probes, inner_basis, inner_transfer, inner_tree)
    coords_b, coords_a = node_halo(coords)
    coarse = coarse_exchange(pay, node)

    wide = width // STEPS
    big = pl.BlockSpec((8, LEAF, wide), lambda i: (0, 0, i))
    flat = pl.BlockSpec((LEAF, wide), lambda i: (0, i))
    stores = [
        pltpu.VMEM((3 * width // LEAF, LEAF, TILE), bf16),
        pltpu.VMEM((3 * width // LEAF, LEAF, TILE), bf16),
        pltpu.VMEM((LEAF, TILE), bf16),
    ]
    middle, next_coords, pay = pl.pallas_call(
        inner_kernel,
        grid=(STEPS,),
        in_specs=[SMEM] * 3 + [VMEM] * 13 + [big, big, flat, flat, flat, flat],
        out_specs=(flat, flat, VMEM),
        out_shape=(struct((LEAF, width), bf16), struct((LEAF, width), bf16), struct((3, LEAF, TILE), bf16)),
        scratch_shapes=stores + [pltpu.VMEM((LEAF, TILE), f32)],
        compiler_params=params(32),
        name="inner",
    )(
        scal, near_table, far_table,
        rows_b, probes, rows_a, coords_b, coords, coords_a,
        *coarse, inner_tree, inner_links, outer_tree,
        inner_near, inner_far, inner_basis, inner_transfer, outer_basis, outer_transfer,
    )
    rows_b, rows_a = node_halo(middle)
    coords_b, coords_a = node_halo(next_coords)
    coarse = coarse_exchange(pay, node)
    samples, gram = pl.pallas_call(
        outer_kernel,
        grid=(STEPS,),
        in_specs=[SMEM] * 3 + [VMEM] * 12 + [big, big, flat, flat],
        out_specs=(flat, VMEM),
        out_shape=(struct((LEAF, width), f32), struct((LEAF, LEAF), f32)),
        scratch_shapes=stores,
        compiler_params=params(32),
        name="outer",
    )(
        scal, near_table, far_table,
        rows_b, middle, rows_a, coords_b, next_coords, coords_a,
        *coarse, outer_tree, outer_links,
        outer_near, outer_far, outer_basis, outer_transfer,
    )
    for mask in (1, 2, 6, 8, 24):
        gram = gram + swap(gram, mask)
    pairs = width // TILE
    pair_basis, work = pl.pallas_call(
        pair_kernel,
        in_specs=[VMEM],
        out_specs=(VMEM, VMEM),
        out_shape=(struct((LEAF, width), f32), struct((pairs, LEAF, TILE), f32)),
        compiler_params=params(32),
        name="pairs",
    )(samples)
    scale = TILE * pairs * lax.axis_size("leaf")
    group_basis = pl.pallas_call(
        lambda *refs: group_kernel(*refs, scale=scale),
        in_specs=[VMEM, VMEM],
        out_specs=VMEM,
        out_shape=struct((LEAF, pairs * LEAF), f32),
        scratch_shapes=[pltpu.VMEM((1, LEAF, TILE), f32)],
        compiler_params=params(32),
        name="group",
    )(gram, work)
    return (pair_basis, group_basis)


def solution(mesh):
    flat = P(None, AXES)
    index = P(AXES, None)
    blocks = P(None, None, AXES)
    tree = P(None, None, None, AXES)
    factor = (blocks, flat, blocks, flat, tree, tree)
    return jax.shard_map(
        local,
        mesh=mesh,
        in_specs=(flat, index, index) + factor + factor,
        out_specs=(flat, flat),
        check_vma=False,
    )
```

```python
import jax
import jax.numpy as jnp
from jax import lax
from jax.experimental import pallas as pl
from jax.experimental.pallas import tpu as pltpu
from jax.sharding import PartitionSpec as P

AXES = ("box", "leaf")
LEAF = 64
TILE = 128
STEPS = 8
bf16 = jnp.bfloat16
f32 = jnp.float32
highest = lax.Precision.HIGHEST

NN = (((1,), (0,)), ((), ()))
NT = (((1,), (1,)), ((), ()))


def dot(a, b, dims=NN, precision=None):
    return lax.dot_general(a, b, dims, precision=precision, preferred_element_type=f32)


def low_half(shape):
    return lax.broadcasted_iota(jnp.int32, shape, len(shape) - 1) < LEAF


def two_blocks(tile):
    low = low_half(tile.shape)
    zero = jnp.zeros_like(tile)
    return jnp.concatenate([jnp.where(low, tile, zero), jnp.where(low, zero, tile)], axis=0)


def swap_halves(tile):
    return jnp.concatenate([tile[:, LEAF:], tile[:, :LEAF]], axis=1)


def twice(block):
    return jnp.concatenate([block, block], axis=1)


def lanes(t):
    return pl.ds(pl.multiple_of(t * TILE, TILE), TILE)


def coarse_payload(sums, tree_ref, scal_ref, pay_ref):
    folded = sums + swap_halves(sums)
    pay_ref[0] = folded.astype(bf16)
    up = dot(folded[:, :LEAF].astype(bf16), tree_ref[0, scal_ref[0]])
    pay_ref[1] = twice(up).astype(bf16)
    up = dot(up.astype(bf16), tree_ref[1, scal_ref[1]])
    pay_ref[2] = twice(up).astype(bf16)


def split(x):
    high = x.astype(bf16)
    return high, (x - high.astype(f32)).astype(bf16)


def dot3(a, b, dims=NN):
    ah, al = split(a)
    bh, bl = split(b)
    side = dims[0][1][0]
    return dot(jnp.concatenate([ah, ah, al], axis=1), jnp.concatenate([bh, bl, bh], axis=side), dims)


def fetch(sources, targets, sems, chunks):
    def piece(n, g):
        source, target = sources[n], targets[n]
        wide = source.shape[-1] // chunks
        at = (slice(None),) * (len(source.shape) - 1) + (pl.ds(g * wide, wide),)
        return pltpu.make_async_copy(source.at[at], target.at[at], sems.at[n, g])

    for g in range(chunks):
        for n in range(len(sources)):
            piece(n, g).start()

    def wait(g):
        for n in range(len(sources)):
            piece(n, g).wait()

    return wait


def coords_kernel(scal_ref, tree_ref, probes_hbm, basis_hbm, transfer_hbm, coords_ref, pay_ref, rows_ref, basis_ref, transfer_ref, sems):
    wait = fetch((probes_hbm, basis_hbm, transfer_hbm), (rows_ref, basis_ref, transfer_ref), sems, STEPS // 2)
    per = rows_ref.shape[1] // TILE // (STEPS // 2)
    for g in range(STEPS // 2):
        wait(g)
        for u in range(per):
            at = slice((g * per + u) * TILE, (g * per + u + 1) * TILE)
            coords_ref[:, at] = dot(rows_ref[:, at], two_blocks(basis_ref[:, at]), NT).astype(bf16)
    coarse_payload(node_sums(coords_ref, transfer_ref), tree_ref, scal_ref, pay_ref)


def node_sums(coords_ref, transfer_ref):
    def step(g, sums):
        for u in range(8):
            at = lanes(g * 8 + u)
            sums = sums + dot(coords_ref[:, at], two_blocks(transfer_ref[:, at]))
        return sums

    return lax.fori_loop(0, coords_ref.shape[1] // TILE // 8, step, jnp.zeros((LEAF, TILE), f32))


def by_tiles(count, one):
    def step(g, carry):
        for u in range(8):
            one(lanes(g * 8 + u))
        return carry

    lax.fori_loop(0, count // 8, step, 0)


def store_tile(store_ref, t, tile):
    store_ref[t] = tile
    store_ref[store_ref.shape[0] // 2 + t] = swap_halves(tile)


def fill_store(store_ref, sources, bases):
    tiles = sources[0].shape[1] // TILE
    for n, (source, basis) in enumerate(zip(sources, bases)):

        def step(g, carry, n=n, source=source, basis=basis):
            for u in range(8):
                t = g * 8 + u
                tile = source[:, lanes(t)]
                if basis is not None:
                    tile = dot(tile, two_blocks(basis[:, lanes(t)]), NT).astype(bf16)
                store_tile(store_ref, n * tiles + t, tile)
            return carry

        lax.fori_loop(0, tiles // 8, step, 0)


def gathered(store_ref, index_ref, pair, low):
    rows = []
    for h in range(2):
        base = (2 * pair + h) * 8
        cols = []
        for k in range(4):
            first = store_ref[index_ref[base + 2 * k]]
            second = store_ref[index_ref[base + 2 * k + 1]]
            cols.append(jnp.where(low, first, second))
        rows.append(jnp.concatenate(cols, axis=1))
    return jnp.concatenate(rows, axis=0)


def interact_kernel(index_ref, before_ref, own_ref, after_ref, *refs):
    *bases, blocks_ref, out_ref, store_ref = refs
    bases = (bases[0], None, bases[1]) if bases else (None, None, None)
    fill_store(store_ref, (before_ref, own_ref, after_ref), bases)
    low = low_half((LEAF, TILE))

    def step(g, carry):
        for u in range(4):
            pair = g * 4 + u
            blocks = blocks_ref[:, :, lanes(pair)].reshape(8 * LEAF, TILE)
            both = dot(gathered(store_ref, index_ref, pair, low), blocks)
            out_ref[:, lanes(pair)] = jnp.where(low, both[:LEAF], both[LEAF:])
        return carry

    lax.fori_loop(0, own_ref.shape[1] // TILE // 4, step, 0)


def descend(scal_ref, mine_ref, other_ref, first_ref, second_ref, tree_ref, links_ref):
    b0, b1, b2 = scal_ref[0], scal_ref[1], scal_ref[2]
    odd, has_left, has_right = scal_ref[3], scal_ref[4], scal_ref[5]

    def low_group(n):
        return jnp.where(b2 == 0, mine_ref[n], other_ref[n])

    def high_group(n):
        return jnp.where(b2 == 0, other_ref[n], mine_ref[n])

    def left(n):
        tile = jnp.where(odd == 1, first_ref[n], second_ref[n])
        return jnp.where(has_left == 1, tile, jnp.zeros_like(tile))

    def right(n):
        tile = jnp.where(odd == 1, second_ref[n], first_ref[n])
        return jnp.where(has_right == 1, tile, jnp.zeros_like(tile))

    def pick(j, options):
        tile = options[-1]
        for n in range(len(options) - 2, -1, -1):
            tile = jnp.where(j == n, options[n], tile)
        return tile

    ext0 = [left(2), low_group(0), low_group(1), high_group(0), high_group(1), right(2)]
    ext1 = [left(1), low_group(2), high_group(2), right(1)]
    j0, j1 = b2 * 2 + b1, b2
    around = [
        (pick(j0, ext0[:4]), pick(j0, ext0[2:])),
        (pick(j1, ext1[:2]), pick(j1, ext1[2:])),
        (left(0), right(0)),
    ]
    coupled = []
    for c, parity in enumerate((b0, b1, b2)):
        mid = links_ref[c, 1]
        none = jnp.zeros_like(mid)
        lo = jnp.concatenate([links_ref[c, 0], jnp.where(parity == 1, mid, none)], axis=0)
        hi = jnp.concatenate([jnp.where(parity == 0, mid, none), links_ref[c, 2]], axis=0)
        coupled.append(dot(around[c][0], lo) + dot(around[c][1], hi))
    h = coupled[1] + dot(coupled[2].astype(bf16), tree_ref[1, b1], NT)
    h = coupled[0] + dot(h.astype(bf16), tree_ref[0, b0], NT)
    return twice(h).astype(bf16)


def finish(near_ref, far_ref, basis_ref, transfer_ref, descent, coeffs_ref, out_ref):
    def coeffs(at):
        down = dot(descent, two_blocks(transfer_ref[:, at]), NT)
        coeffs_ref[:, at] = (far_ref[:, at] + down).astype(bf16)

    def result(at):
        out = near_ref[:, at] + dot(coeffs_ref[:, at], two_blocks(basis_ref[:, at]))
        out_ref[:, at] = out.astype(out_ref.dtype)

    count = near_ref.shape[1] // TILE
    by_tiles(count, coeffs)
    by_tiles(count, result)


def inner_kernel(
    scal_ref, near_ref, far_ref, basis_ref, transfer_ref,
    mine_ref, other_ref, first_ref, second_ref, tree_ref, links_ref, next_tree_ref, next_basis_ref, next_transfer_ref,
    middle_ref, coords_ref, pay_ref, coeffs_ref,
):
    descent = descend(scal_ref, mine_ref, other_ref, first_ref, second_ref, tree_ref, links_ref)
    finish(near_ref, far_ref, basis_ref, transfer_ref, descent, coeffs_ref, middle_ref)

    def next_coords(at):
        coords_ref[:, at] = dot(middle_ref[:, at], two_blocks(next_basis_ref[:, at]), NT).astype(bf16)

    by_tiles(middle_ref.shape[1] // TILE, next_coords)
    coarse_payload(node_sums(coords_ref, next_transfer_ref), next_tree_ref, scal_ref, pay_ref)


def outer_kernel(
    scal_ref, near_ref, far_ref, basis_ref, transfer_ref,
    mine_ref, other_ref, first_ref, second_ref, tree_ref, links_ref,
    samples_ref, work_ref, gram_ref, coeffs_ref,
):
    descent = descend(scal_ref, mine_ref, other_ref, first_ref, second_ref, tree_ref, links_ref)
    finish(near_ref, far_ref, basis_ref, transfer_ref, descent, coeffs_ref, samples_ref)
    low = low_half((LEAF, TILE))

    def step(g, total):
        for u in range(4):
            t = g * 4 + u
            both = jnp.concatenate([samples_ref[:, lanes(2 * t)], samples_ref[:, lanes(2 * t + 1)]], axis=0)
            both = dot3(both, both, NT)
            gram = jnp.where(low, both[:LEAF], both[LEAF:]) / TILE
            work_ref[t] = gram
            total = total + gram
        return total

    total = lax.fori_loop(0, work_ref.shape[0] // 4, step, jnp.zeros((LEAF, TILE), f32))
    gram_ref[...] = total + swap_halves(total)


def lane_take(tile, index):
    return jnp.take_along_axis(tile, index, axis=1, mode="promise_in_bounds")


def each(count, unroll, one):
    unroll = min(unroll, count)

    def step(g, carry):
        for u in range(unroll):
            one(g * unroll + u)
        return carry

    lax.fori_loop(0, count // unroll, step, 0)


def eliminate(work_ref, tee_ref):
    count = work_ref.shape[0]
    per = min(count, 4)
    groups = count // per
    sub = lax.broadcasted_iota(jnp.int32, (8, TILE), 0)
    lane = lax.broadcasted_iota(jnp.int32, (8, TILE), 1)
    col, half = lane % LEAF, lane // LEAF
    panels = LEAF // 8
    for kb in range(panels):
        base = kb * 8
        rows = slice(base, base + 8)
        inside = (col >= base) & (col < base + 8)
        cols = []
        for g in range(groups):
            tiles = [work_ref[g * per + t, rows, :] for t in range(per)]
            packed = []
            for j in range(8):
                index = lane // 16 % 2 * LEAF + (base + j)
                value = lane_take(tiles[0], index)
                for t in range(1, per):
                    value = jnp.where(lane // 32 == t, lane_take(tiles[t], index), value)
                packed.append(value)
            cols.append(packed)
        tees = [[] for _ in range(groups)]
        for j in range(8):
            for c, tee in zip(cols, tees):
                inv = lax.rsqrt(c[j][j : j + 1, :])
                lower = c[j] * inv
                below = jnp.where(sub > j, lower, 0.0)
                for n in range(j + 1, 8):
                    c[n] = c[n] - lower * lower[n : n + 1, :]
                for n in range(j):
                    row = tee[n][j : j + 1, :] * inv
                    tee[n] = jnp.where(sub == j, row, tee[n] - below * row)
                tee.append(jnp.where(sub == j, inv, -below * inv))
        for g in range(groups):
            for j in range(8):
                tee_ref[g * 8 + j] = tees[g][j]

        for tt in range(per):
            index = tt * 32 + half * 16
            for g in range(groups):
                t = g * per + tt
                panel = work_ref[t, rows, :]
                spread = [lane_take(tee_ref[g * 8 + j], index) for j in range(8)]
                done = spread[0] * panel[:1, :]
                for j in range(1, 8):
                    done = done + spread[j] * panel[j : j + 1, :]
                for j in range(8):
                    done = jnp.where((col == base + j) & (sub >= j), spread[j], done)
                work_ref[t, rows, :] = done
        if kb == panels - 1:
            break

        def update(t):
            left = work_ref[t, rows, :]
            right = jnp.where(inside & (col > base + sub), 0.0, left)
            left = stacked(left, (0, 0, 1))
            right = stacked(right, (0, 1, 0))
            both = lax.dot_general(left, right, (((0,), (0,)), ((), ())), preferred_element_type=f32)
            for ib in range(kb + 1, panels):
                at = slice(ib * 8, ib * 8 + 8)
                other = slice(LEAF + ib * 8, LEAF + ib * 8 + 8)
                rest = jnp.where(inside, 0.0, work_ref[t, at, :])
                work_ref[t, at, :] = rest - jnp.where(half == 0, both[at], both[other])

        each(count, 4, update)


def stacked(x, order):
    high = x.astype(bf16).astype(f32)
    pieces = (high, x - high)
    return jnp.concatenate([pieces[n] for n in order] + [jnp.zeros_like(x)], axis=0).astype(bf16)


def parts(tile):
    row = lax.broadcasted_iota(jnp.int32, tile.shape, 0)
    col = lax.broadcasted_iota(jnp.int32, tile.shape, 1) % LEAF
    return row, col


def pair_kernel(gram_ref, samples_ref, work_ref, basis_ref, *scratch):
    work_ref[...] = gram_ref[...]
    eliminate(work_ref, *scratch)

    def solve(t):
        tile = work_ref[t]
        row, col = parts(tile)
        inverse = two_blocks(jnp.where(col <= row, tile, 0.0))
        one, two = lanes(2 * t), lanes(2 * t + 1)
        solved = dot3(inverse, jnp.concatenate([samples_ref[:, one], samples_ref[:, two]], axis=0))
        basis_ref[:, one] = solved[:LEAF]
        basis_ref[:, two] = solved[LEAF:]

    each(work_ref.shape[0], 4, solve)


def group_kernel(gram_ref, work_ref, out_ref, own_ref, *scratch, scale):
    own_ref[0] = gram_ref[...] / scale
    eliminate(own_ref, *scratch)
    tile = own_ref[0]
    row, col = parts(tile)
    inverse = jnp.where(col <= row, tile, 0.0)

    def solve(t):
        tile = work_ref[t]
        upper = jnp.where(col > row, tile, jnp.where(col == row, 1.0 / tile, 0.0))
        out_ref[:, lanes(t)] = dot3(inverse, two_blocks(upper), NT)

    each(work_ref.shape[0], 4, solve)


HBM = pl.BlockSpec(memory_space=pltpu.HBM)
VMEM = pl.BlockSpec(memory_space=pltpu.VMEM)
SMEM = pl.BlockSpec(memory_space=pltpu.SMEM)


def params(mib):
    return pltpu.CompilerParams(vmem_limit_bytes=mib * 2**20)


def elimination(count):
    return [
        pltpu.VMEM((max(count // 4, 1) * 8, 8, TILE), f32),
    ]


def struct(shape, dtype):
    return jax.ShapeDtypeStruct(shape, dtype)


def swap(x, mask):
    count = lax.axis_size(AXES)
    return lax.ppermute(x, AXES, [(i, i ^ mask) for i in range(count)])


def neighbours(x, width, second):
    count = lax.axis_size(AXES)
    blocks = count // width
    route = []
    for b in range(blocks):
        forward = (b % 2 == 0) != second
        to = (b + 1 if forward else b - 1) % blocks
        route += [(b * width + m, to * width + m) for m in range(width)]
    return lax.ppermute(x, AXES, route)


def node_halo(x):
    count = lax.axis_size(AXES)
    route = [(i, (i - 1 if i % 2 == 0 else i + 1) % count) for i in range(count)]
    return lax.ppermute(x, AXES, route), swap(x, 1)


def leaf_table(index, node):
    leaves = index.shape[0]
    place = index - (node - 1) * leaves
    block = place // leaves
    block = jnp.where(node % 2 == 1, 2 - block, block)
    place = block * leaves + place % leaves
    slot = lax.broadcasted_iota(jnp.int32, index.shape, 1)
    return (((place + slot) % 2) * (3 * leaves // 2) + place // 2).reshape(-1)


def coarse_near(pay, node):
    low = low_half((LEAF, TILE))
    b0, b1 = node % 2, node // 2 % 2

    def halves(bit, mine, other):
        return jnp.where(low == (bit == 0), mine, other)

    other = swap(pay, 1)
    z0 = halves(b0, pay[0], other[0])
    stage = jnp.stack([z0, pay[1] + other[1], pay[2] + other[2]])
    other = swap(stage, 2)
    first = jnp.where(b1 == 0, stage[0], other[0])
    second = jnp.where(b1 == 0, other[0], stage[0])
    return jnp.stack([first, second, halves(b1, stage[1], other[1]), stage[2] + other[2]])


def coarse_far(mine, other, node):
    low = low_half((LEAF, TILE))
    b2, odd = node // 4 % 2, node // 8 % 2
    top = jnp.where(low == (b2 == 0), mine[3], other[3])
    lo = jnp.where(b2 == 0, mine, other)
    hi = jnp.where(b2 == 0, other, mine)
    rightward = jnp.stack([top, hi[2], hi[1]])
    leftward = jnp.stack([top, lo[2], lo[0]])
    one = neighbours(jnp.where(odd == 0, rightward, leftward), 8, False)
    two = neighbours(jnp.where(odd == 0, leftward, rightward), 8, True)
    return one, two


def after(x, *values):
    return lax.optimization_barrier((x, *values))[0]


def local(
    probes,
    near_index,
    far_index,
    inner_near,
    inner_basis,
    inner_far,
    inner_transfer,
    inner_tree,
    inner_links,
    outer_near,
    outer_basis,
    outer_far,
    outer_transfer,
    outer_tree,
    outer_links,
):
    node = lax.axis_index(AXES)
    count = lax.axis_size(AXES)
    width = probes.shape[1]
    block = node // 8
    scal = jnp.stack(
        [
            node % 2,
            node // 2 % 2,
            node // 4 % 2,
            block % 2,
            (block > 0).astype(jnp.int32),
            (block < count // 8 - 1).astype(jnp.int32),
        ]
    ).astype(jnp.int32)
    near_table = leaf_table(near_index, node)
    far_table = leaf_table(far_index, node)

    def interact(index, rows, blocks, bases=()):
        return pl.pallas_call(
            interact_kernel,
            in_specs=[SMEM] + [VMEM] * (4 + len(bases)),
            out_specs=VMEM,
            out_shape=struct((LEAF, width), f32),
            scratch_shapes=[pltpu.VMEM((3 * width // LEAF, LEAF, TILE), bf16)],
            compiler_params=params(6),
            name="interact",
        )(index, *rows, *bases, blocks)

    row = struct((LEAF, width), bf16)
    payload = struct((3, LEAF, TILE), bf16)
    pairs = width // TILE

    rows_b, rows_a = node_halo(probes)
    coords, pay, rows, basis, transfer = pl.pallas_call(
        coords_kernel,
        in_specs=[SMEM, VMEM, HBM, HBM, HBM],
        out_specs=(VMEM,) * 5,
        out_shape=(row, payload, row, row, row),
        scratch_shapes=[pltpu.SemaphoreType.DMA((3, STEPS // 2))],
        compiler_params=params(56),
        name="coords",
    )(scal, inner_tree, probes, inner_basis, inner_transfer)
    mine = coarse_near(pay, node)
    other = swap(mine, 6)
    coords_b, coords_a = node_halo(after(coords, mine))
    one, two = coarse_far(mine, other, node)
    basis_b, basis_a = node_halo(after(outer_basis, other))
    near_part = interact(near_table, (rows_b, rows, rows_a), inner_near)
    far_part = interact(far_table, (coords_b, coords, coords_a), inner_far)
    far_part, basis_b, basis_a = lax.optimization_barrier((far_part, basis_b, basis_a))
    middle, coords, pay = pl.pallas_call(
        inner_kernel,
        in_specs=[SMEM] + [VMEM] * 13,
        out_specs=(VMEM,) * 3,
        out_shape=(row, row, payload),
        scratch_shapes=[pltpu.VMEM((LEAF, width), bf16)],
        compiler_params=params(6),
        name="inner",
    )(
        scal, near_part, far_part, basis, transfer,
        mine, other, one, two, inner_tree, inner_links, outer_tree, outer_basis, outer_transfer,
    )
    middle_b, middle_a = node_halo(middle)
    mine = coarse_near(pay, node)
    other = swap(mine, 6)
    one, two = coarse_far(mine, other, node)
    near_part = interact(near_table, (middle_b, middle, middle_a), outer_near)
    far_part = interact(far_table, (middle_b, coords, middle_a), outer_far, (basis_b, basis_a))
    samples, grams, gram = pl.pallas_call(
        outer_kernel,
        in_specs=[SMEM] + [VMEM] * 10,
        out_specs=(VMEM,) * 3,
        out_shape=(
            struct((LEAF, width), f32),
            struct((pairs // 2, LEAF, TILE), f32),
            struct((LEAF, TILE), f32),
        ),
        scratch_shapes=[pltpu.VMEM((LEAF, width), bf16)],
        compiler_params=params(6),
        name="outer",
    )(scal, near_part, far_part, outer_basis, outer_transfer, mine, other, one, two, outer_tree, outer_links)
    for mask in (1, 2, 6, 8, 24):
        gram = gram + swap(gram, mask)
    work, pair_basis = pl.pallas_call(
        pair_kernel,
        in_specs=[VMEM, VMEM],
        out_specs=(VMEM, VMEM),
        out_shape=(struct(grams.shape, f32), struct((LEAF, width), f32)),
        scratch_shapes=elimination(pairs // 2),
        compiler_params=params(6),
        name="pairs",
    )(grams, samples)
    scale = pairs * lax.axis_size("leaf")
    group_basis = pl.pallas_call(
        lambda *refs: group_kernel(*refs, scale=scale),
        in_specs=[VMEM, VMEM],
        out_specs=VMEM,
        out_shape=struct((LEAF, pairs * LEAF), f32),
        scratch_shapes=[pltpu.VMEM((1, LEAF, TILE), f32)] + elimination(1),
        compiler_params=params(6),
        name="group",
    )(gram, work)
    return (pair_basis, group_basis)


def solution(mesh):
    flat = P(None, AXES)
    index = P(AXES, None)
    blocks = P(None, None, AXES)
    tree = P(None, None, None, AXES)
    factor = (blocks, flat, blocks, flat, tree, tree)
    return jax.shard_map(
        local,
        mesh=mesh,
        in_specs=(flat, index, index) + factor + factor,
        out_specs=(flat, flat),
        check_vma=False,
    )
```

```python
import jax
import jax.numpy as jnp
from jax import lax
from jax.experimental import pallas as pl
from jax.experimental.pallas import tpu as pltpu
from jax.sharding import PartitionSpec as P

AXES = ("box", "leaf")
LEAF = 64
TILE = 128
STEPS = 8
STREAM = (True, False)
bf16 = jnp.bfloat16
f32 = jnp.float32
highest = lax.Precision.HIGHEST

NN = (((1,), (0,)), ((), ()))
NT = (((1,), (1,)), ((), ()))


def dot(a, b, dims=NN, precision=None):
    return lax.dot_general(a, b, dims, precision=precision, preferred_element_type=f32)


def low_half(shape):
    return lax.broadcasted_iota(jnp.int32, shape, len(shape) - 1) < LEAF


def two_blocks(tile):
    low = low_half(tile.shape)
    zero = jnp.zeros_like(tile)
    return jnp.concatenate([jnp.where(low, tile, zero), jnp.where(low, zero, tile)], axis=0)


def swap_halves(tile):
    return jnp.concatenate([tile[:, LEAF:], tile[:, :LEAF]], axis=1)


def twice(block):
    return jnp.concatenate([block, block], axis=1)


def lanes(t):
    return pl.ds(pl.multiple_of(t * TILE, TILE), TILE)


def coarse_payload(sums, tree_ref, scal_ref, pay_ref):
    folded = sums + swap_halves(sums)
    pay_ref[0] = folded.astype(bf16)
    up = dot(folded[:, :LEAF].astype(bf16), tree_ref[0, scal_ref[0]])
    pay_ref[1] = twice(up).astype(bf16)
    up = dot(up.astype(bf16), tree_ref[1, scal_ref[1]])
    pay_ref[2] = twice(up).astype(bf16)


def split(x):
    high = x.astype(bf16)
    return high, (x - high.astype(f32)).astype(bf16)


def dot3(a, b, dims=NN):
    ah, al = split(a)
    bh, bl = split(b)
    side = dims[0][1][0]
    return dot(jnp.concatenate([ah, ah, al], axis=1), jnp.concatenate([bh, bl, bh], axis=side), dims)


def fetch(sources, targets, sems, chunks):
    def piece(n, g):
        source, target = sources[n], targets[n]
        wide = source.shape[-1] // chunks
        at = (slice(None),) * (len(source.shape) - 1) + (pl.ds(g * wide, wide),)
        return pltpu.make_async_copy(source.at[at], target.at[at], sems.at[n, g])

    for g in range(chunks):
        for n in range(len(sources)):
            piece(n, g).start()

    def wait(g):
        for n in range(len(sources)):
            piece(n, g).wait()

    return wait


def coords_kernel(scal_ref, tree_ref, probes_hbm, basis_hbm, transfer_hbm, coords_ref, pay_ref, rows_ref, basis_ref, transfer_ref, sems):
    wait = fetch((probes_hbm, basis_hbm, transfer_hbm), (rows_ref, basis_ref, transfer_ref), sems, STEPS // 2)
    per = rows_ref.shape[1] // TILE // (STEPS // 2)
    for g in range(STEPS // 2):
        wait(g)
        for u in range(per):
            at = slice((g * per + u) * TILE, (g * per + u + 1) * TILE)
            coords_ref[:, at] = dot(rows_ref[:, at], two_blocks(basis_ref[:, at]), NT).astype(bf16)
    coarse_payload(node_sums(coords_ref, transfer_ref), tree_ref, scal_ref, pay_ref)


def node_sums(coords_ref, transfer_ref):
    def step(g, sums):
        for u in range(8):
            at = lanes(g * 8 + u)
            sums = sums + dot(coords_ref[:, at], two_blocks(transfer_ref[:, at]))
        return sums

    return lax.fori_loop(0, coords_ref.shape[1] // TILE // 8, step, jnp.zeros((LEAF, TILE), f32))


def by_tiles(count, one):
    def step(g, carry):
        for u in range(8):
            one(lanes(g * 8 + u))
        return carry

    lax.fori_loop(0, count // 8, step, 0)


def store_tile(store_ref, t, tile):
    store_ref[t] = tile
    store_ref[store_ref.shape[0] // 2 + t] = swap_halves(tile)


def fill_store(store_ref, sources, bases):
    tiles = sources[0].shape[1] // TILE
    for n, (source, basis) in enumerate(zip(sources, bases)):

        def step(g, carry, n=n, source=source, basis=basis):
            for u in range(8):
                t = g * 8 + u
                tile = source[:, lanes(t)]
                if basis is not None:
                    tile = dot(tile, two_blocks(basis[:, lanes(t)]), NT).astype(bf16)
                store_tile(store_ref, n * tiles + t, tile)
            return carry

        lax.fori_loop(0, tiles // 8, step, 0)


def gathered(store_ref, index_ref, pair, low):
    rows = []
    for h in range(2):
        base = (2 * pair + h) * 8
        cols = []
        for k in range(4):
            first = store_ref[index_ref[base + 2 * k]]
            second = store_ref[index_ref[base + 2 * k + 1]]
            cols.append(jnp.where(low, first, second))
        rows.append(jnp.concatenate(cols, axis=1))
    return jnp.concatenate(rows, axis=0)


def interact_kernel(index_ref, before_ref, own_ref, after_ref, *refs, streamed):
    if streamed:
        *bases, blocks_hbm, out_ref, store_ref, blocks_ref, sems = refs
        wide = blocks_ref.shape[2] // STEPS

        def piece(g):
            at = (slice(None), slice(None), pl.ds(pl.multiple_of(g * wide, wide), wide))
            return pltpu.make_async_copy(blocks_hbm.at[at], blocks_ref.at[at], sems.at[g])

        for g in range(STEPS):
            piece(g).start()
    else:
        *bases, blocks_ref, out_ref, store_ref = refs
    bases = (bases[0], None, bases[1]) if bases else (None, None, None)
    fill_store(store_ref, (before_ref, own_ref, after_ref), bases)
    low = low_half((LEAF, TILE))
    per = own_ref.shape[1] // TILE // STEPS

    def step(g, carry):
        if streamed:
            piece(g).wait()
        for u in range(per):
            pair = g * per + u
            blocks = blocks_ref[:, :, lanes(pair)].reshape(8 * LEAF, TILE)
            both = dot(gathered(store_ref, index_ref, pair, low), blocks)
            out_ref[:, lanes(pair)] = jnp.where(low, both[:LEAF], both[LEAF:])
        return carry

    lax.fori_loop(0, STEPS, step, 0)


def descend(scal_ref, mine_ref, other_ref, first_ref, second_ref, tree_ref, links_ref):
    b0, b1, b2 = scal_ref[0], scal_ref[1], scal_ref[2]
    odd, has_left, has_right = scal_ref[3], scal_ref[4], scal_ref[5]

    def low_group(n):
        return jnp.where(b2 == 0, mine_ref[n], other_ref[n])

    def high_group(n):
        return jnp.where(b2 == 0, other_ref[n], mine_ref[n])

    crossed = (odd == 1) == (b0 == 0)

    def left(n):
        tile = jnp.where(crossed, first_ref[n], second_ref[n])
        return jnp.where(has_left == 1, tile, jnp.zeros_like(tile))

    def right(n):
        tile = jnp.where(crossed, second_ref[n], first_ref[n])
        return jnp.where(has_right == 1, tile, jnp.zeros_like(tile))

    def pick(j, options):
        tile = options[-1]
        for n in range(len(options) - 2, -1, -1):
            tile = jnp.where(j == n, options[n], tile)
        return tile

    ext0 = [left(2), low_group(0), low_group(1), high_group(0), high_group(1), right(2)]
    ext1 = [left(1), low_group(2), high_group(2), right(1)]
    j0, j1 = b2 * 2 + b1, b2
    around = [
        (pick(j0, ext0[:4]), pick(j0, ext0[2:])),
        (pick(j1, ext1[:2]), pick(j1, ext1[2:])),
        (left(0), right(0)),
    ]
    coupled = []
    for c, parity in enumerate((b0, b1, b2)):
        mid = links_ref[c, 1]
        none = jnp.zeros_like(mid)
        lo = jnp.concatenate([links_ref[c, 0], jnp.where(parity == 1, mid, none)], axis=0)
        hi = jnp.concatenate([jnp.where(parity == 0, mid, none), links_ref[c, 2]], axis=0)
        coupled.append(dot(around[c][0], lo) + dot(around[c][1], hi))
    h = coupled[1] + dot(coupled[2].astype(bf16), tree_ref[1, b1], NT)
    h = coupled[0] + dot(h.astype(bf16), tree_ref[0, b0], NT)
    return twice(h).astype(bf16)


def finish(near_ref, far_ref, basis_ref, transfer_ref, descent, coeffs_ref, out_ref):
    def coeffs(at):
        down = dot(descent, two_blocks(transfer_ref[:, at]), NT)
        coeffs_ref[:, at] = (far_ref[:, at] + down).astype(bf16)

    def result(at):
        out = near_ref[:, at] + dot(coeffs_ref[:, at], two_blocks(basis_ref[:, at]))
        out_ref[:, at] = out.astype(out_ref.dtype)

    count = near_ref.shape[1] // TILE
    by_tiles(count, coeffs)
    by_tiles(count, result)


def inner_kernel(
    scal_ref, near_ref, far_ref, basis_ref, transfer_ref,
    mine_ref, other_ref, first_ref, second_ref, tree_ref, links_ref,
    middle_ref, coeffs_ref,
):
    descent = descend(scal_ref, mine_ref, other_ref, first_ref, second_ref, tree_ref, links_ref)
    finish(near_ref, far_ref, basis_ref, transfer_ref, descent, coeffs_ref, middle_ref)


def next_kernel(scal_ref, tree_ref, rows_ref, basis_ref, transfer_ref, coords_ref, pay_ref):
    def coords(at):
        coords_ref[:, at] = dot(rows_ref[:, at], two_blocks(basis_ref[:, at]), NT).astype(bf16)

    by_tiles(rows_ref.shape[1] // TILE, coords)
    coarse_payload(node_sums(coords_ref, transfer_ref), tree_ref, scal_ref, pay_ref)


def outer_kernel(
    scal_ref, near_ref, far_ref, basis_ref, transfer_ref,
    mine_ref, other_ref, first_ref, second_ref, tree_ref, links_ref,
    samples_ref, work_ref, gram_ref, coeffs_ref,
):
    descent = descend(scal_ref, mine_ref, other_ref, first_ref, second_ref, tree_ref, links_ref)
    finish(near_ref, far_ref, basis_ref, transfer_ref, descent, coeffs_ref, samples_ref)
    low = low_half((LEAF, TILE))

    def step(g, total):
        for u in range(4):
            t = g * 4 + u
            both = jnp.concatenate([samples_ref[:, lanes(2 * t)], samples_ref[:, lanes(2 * t + 1)]], axis=0)
            both = dot3(both, both, NT)
            gram = jnp.where(low, both[:LEAF], both[LEAF:]) / TILE
            work_ref[t] = gram
            total = total + gram
        return total

    total = lax.fori_loop(0, work_ref.shape[0] // 4, step, jnp.zeros((LEAF, TILE), f32))
    gram_ref[...] = total + swap_halves(total)


def lane_take(tile, index):
    return jnp.take_along_axis(tile, index, axis=1, mode="promise_in_bounds")


def each(count, unroll, one):
    unroll = min(unroll, count)

    def step(g, carry):
        for u in range(unroll):
            one(g * unroll + u)
        return carry

    lax.fori_loop(0, count // unroll, step, 0)


def eliminate(work_ref, tee_ref, first=0, last=LEAF // 8):
    count = work_ref.shape[0]
    per = min(count, 4)
    groups = count // per
    sub = lax.broadcasted_iota(jnp.int32, (8, TILE), 0)
    lane = lax.broadcasted_iota(jnp.int32, (8, TILE), 1)
    col, half = lane % LEAF, lane // LEAF
    panels = LEAF // 8
    for kb in range(first, last):
        base = kb * 8
        rows = slice(base, base + 8)
        inside = (col >= base) & (col < base + 8)
        cols = []
        for g in range(groups):
            tiles = [work_ref[g * per + t, rows, :] for t in range(per)]
            packed = []
            for j in range(8):
                index = lane // 16 % 2 * LEAF + (base + j)
                value = lane_take(tiles[0], index)
                for t in range(1, per):
                    value = jnp.where(lane // 32 == t, lane_take(tiles[t], index), value)
                packed.append(value)
            cols.append(packed)
        tees = [[] for _ in range(groups)]
        for j in range(8):
            for c, tee in zip(cols, tees):
                inv = lax.rsqrt(c[j][j : j + 1, :])
                lower = c[j] * inv
                below = jnp.where(sub > j, lower, 0.0)
                for n in range(j + 1, 8):
                    c[n] = c[n] - lower * lower[n : n + 1, :]
                for n in range(j):
                    row = tee[n][j : j + 1, :] * inv
                    tee[n] = jnp.where(sub == j, row, tee[n] - below * row)
                tee.append(jnp.where(sub == j, inv, -below * inv))
        for g in range(groups):
            for j in range(8):
                tee_ref[g * 8 + j] = tees[g][j]

        for tt in range(per):
            index = tt * 32 + half * 16
            for g in range(groups):
                t = g * per + tt
                panel = work_ref[t, rows, :]
                spread = [lane_take(tee_ref[g * 8 + j], index) for j in range(8)]
                done = spread[0] * panel[:1, :]
                for j in range(1, 8):
                    done = done + spread[j] * panel[j : j + 1, :]
                for j in range(8):
                    done = jnp.where((col == base + j) & (sub >= j), spread[j], done)
                work_ref[t, rows, :] = done
        if kb == panels - 1:
            break

        rest_rows = LEAF - base - 8

        def update(t):
            left = work_ref[t, rows, :]
            right = jnp.where(inside & (col > base + sub), 0.0, left)
            turned = stacked(left, (0, 0, 1)).T.astype(bf16)
            turned = jnp.concatenate([turned[base + 8 : LEAF], turned[LEAF + base + 8 :]], axis=0)
            both = dot(turned, stacked(right, (0, 1, 0)).astype(bf16))
            for ib in range(kb + 1, panels):
                at = slice(ib * 8, ib * 8 + 8)
                n = (ib - kb - 1) * 8
                rest = jnp.where(inside, 0.0, work_ref[t, at, :])
                work_ref[t, at, :] = rest - jnp.where(half == 0, both[n : n + 8], both[rest_rows + n : rest_rows + n + 8])

        each(count, 4, update)


def stacked(x, order):
    high = x.astype(bf16).astype(f32)
    pieces = (high, x - high)
    return jnp.concatenate([pieces[n] for n in order] + [jnp.zeros_like(x)], axis=0)


def parts(tile):
    row = lax.broadcasted_iota(jnp.int32, tile.shape, 0)
    col = lax.broadcasted_iota(jnp.int32, tile.shape, 1) % LEAF
    return row, col


def pair_kernel(before_ref, work_ref, tee_ref, *, first, last):
    work_ref[...] = before_ref[...]
    eliminate(work_ref, tee_ref, first, last)


def solve_kernel(work_ref, samples_ref, basis_ref):
    def solve(t):
        tile = work_ref[t]
        row, col = parts(tile)
        inverse = two_blocks(jnp.where(col <= row, tile, 0.0))
        one, two = lanes(2 * t), lanes(2 * t + 1)
        solved = dot3(inverse, jnp.concatenate([samples_ref[:, one], samples_ref[:, two]], axis=0))
        basis_ref[:, one] = solved[:LEAF]
        basis_ref[:, two] = solved[LEAF:]

    each(work_ref.shape[0], 4, solve)


def eliminate_few(load, save, count):
    shape = (count, 8, TILE)
    sub = lax.broadcasted_iota(jnp.int32, shape, 1)
    lane = lax.broadcasted_iota(jnp.int32, shape, 2)
    low = lane < LEAF
    col = lane % LEAF
    panels = LEAF // 8
    for kb in range(panels):
        panel = load(kb)
        cols = []
        for j in range(8):
            k = kb * 8 + j
            one = jnp.broadcast_to(panel[:, :, k : k + 1], shape)
            two = jnp.broadcast_to(panel[:, :, LEAF + k : LEAF + k + 1], shape)
            cols.append(jnp.where(low, one, two))
        rows = []
        for j in range(8):
            k = kb * 8 + j
            inv = lax.rsqrt(cols[j][:, j : j + 1, :])
            lower = cols[j] * inv
            for n in range(j + 1, 8):
                cols[n] = cols[n] - lower * lower[:, n : n + 1, :]
            row = jnp.where(col[:, :1] == k, inv, panel[:, j : j + 1, :] * inv)
            below = sub > j
            kept = jnp.where(below & (col == k), 0.0, panel)
            panel = jnp.where(sub == j, row, kept - jnp.where(below, lower, 0.0) * row)
            rows.append(row)
        save(kb, panel)
        if kb == panels - 1:
            break
        turned = jnp.swapaxes(panel, 1, 2)
        inside = (col >= kb * 8) & (col < kb * 8 + 8)
        for j in range(8):
            k = kb * 8 + j
            rows[j] = jnp.where((col[:, :1] > k) & (col[:, :1] < kb * 8 + 8), 0.0, rows[j])
        for ib in range(kb + 1, panels):
            rest = jnp.where(inside, 0.0, load(ib))
            for j in range(8):
                one = jnp.broadcast_to(turned[:, ib * 8 : ib * 8 + 8, j : j + 1], shape)
                two = jnp.broadcast_to(turned[:, LEAF + ib * 8 : LEAF + ib * 8 + 8, j : j + 1], shape)
                rest = rest - jnp.where(low, one, two) * rows[j]
            save(ib, rest)


def group_kernel(gram_ref, work_ref, out_ref, own_ref, *, scale):
    own_ref[0] = gram_ref[...] / scale

    def load(b):
        return own_ref[:, b * 8 : b * 8 + 8, :]

    def save(b, value):
        own_ref[:, b * 8 : b * 8 + 8, :] = value

    eliminate_few(load, save, 1)
    tile = own_ref[0]
    row, col = parts(tile)
    inverse = jnp.where(col <= row, tile, 0.0)

    def solve(t):
        tile = work_ref[t]
        upper = jnp.where(col > row, tile, jnp.where(col == row, 1.0 / tile, 0.0))
        out_ref[:, lanes(t)] = dot3(inverse, two_blocks(upper), NT)

    each(work_ref.shape[0], 4, solve)


HBM = pl.BlockSpec(memory_space=pltpu.HBM)
VMEM = pl.BlockSpec(memory_space=pltpu.VMEM)
SMEM = pl.BlockSpec(memory_space=pltpu.SMEM)


def params(mib):
    return pltpu.CompilerParams(vmem_limit_bytes=mib * 2**20)


def elimination(count):
    return [
        pltpu.VMEM((max(count // 4, 1) * 8, 8, TILE), f32),
    ]


def struct(shape, dtype):
    return jax.ShapeDtypeStruct(shape, dtype)


def swap(x, mask):
    count = lax.axis_size(AXES)
    return lax.ppermute(x, AXES, [(i, i ^ mask) for i in range(count)])


def adjacent_rows(x):
    count = lax.axis_size(AXES)
    route = []
    for i in range(count):
        forward = (i // 8 % 2 == 0) == (i % 2 == 0)
        route.append((i, (i + 8 if forward else i - 8) % count))
    return lax.ppermute(x, AXES, route)


def node_halo(x):
    count = lax.axis_size(AXES)
    route = [(i, (i - 1 if i % 2 == 0 else i + 1) % count) for i in range(count)]
    return lax.ppermute(x, AXES, route), swap(x, 1)


def leaf_table(index, node):
    leaves = index.shape[0]
    place = index - (node - 1) * leaves
    block = place // leaves
    block = jnp.where(node % 2 == 1, 2 - block, block)
    place = block * leaves + place % leaves
    slot = lax.broadcasted_iota(jnp.int32, index.shape, 1)
    return (((place + slot) % 2) * (3 * leaves // 2) + place // 2).reshape(-1)


def coarse_near(pay, node):
    low = low_half((LEAF, TILE))
    b0, b1 = node % 2, node // 2 % 2

    def halves(bit, mine, other):
        return jnp.where(low == (bit == 0), mine, other)

    other = swap(pay, 1)
    z0 = halves(b0, pay[0], other[0])
    stage = jnp.stack([z0, pay[1] + other[1], pay[2] + other[2]])
    other = swap(stage, 2)
    first = jnp.where(b1 == 0, stage[0], other[0])
    second = jnp.where(b1 == 0, other[0], stage[0])
    return jnp.stack([first, second, halves(b1, stage[1], other[1]), stage[2] + other[2]])


def far_payload(mine, other, node):
    low = low_half((LEAF, TILE))
    b2, odd = node // 4 % 2, node // 8 % 2
    top = jnp.where(low == (b2 == 0), mine[3], other[3])
    lo = jnp.where(b2 == 0, mine, other)
    hi = jnp.where(b2 == 0, other, mine)
    rightward = jnp.stack([top, hi[2], hi[1]])
    leftward = jnp.stack([top, lo[2], lo[0]])
    return jnp.where((odd == 0) == (node % 2 == 0), rightward, leftward)


def after(x, *values):
    return lax.optimization_barrier((x, *values))[0]


def local(
    probes,
    near_index,
    far_index,
    inner_near,
    inner_basis,
    inner_far,
    inner_transfer,
    inner_tree,
    inner_links,
    outer_near,
    outer_basis,
    outer_far,
    outer_transfer,
    outer_tree,
    outer_links,
):
    node = lax.axis_index(AXES)
    count = lax.axis_size(AXES)
    width = probes.shape[1]
    block = node // 8
    scal = jnp.stack(
        [
            node % 2,
            node // 2 % 2,
            node // 4 % 2,
            block % 2,
            (block > 0).astype(jnp.int32),
            (block < count // 8 - 1).astype(jnp.int32),
        ]
    ).astype(jnp.int32)
    near_table = leaf_table(near_index, node)
    far_table = leaf_table(far_index, node)

    def interact(index, rows, blocks, bases=(), streamed=False):
        scratch = [pltpu.VMEM((3 * width // LEAF, LEAF, TILE), bf16)]
        if streamed:
            scratch += [pltpu.VMEM(blocks.shape, bf16), pltpu.SemaphoreType.DMA((STEPS,))]
        return pl.pallas_call(
            lambda *refs: interact_kernel(*refs, streamed=streamed),
            in_specs=[SMEM] + [VMEM] * (3 + len(bases)) + [HBM if streamed else VMEM],
            out_specs=VMEM,
            out_shape=struct((LEAF, width), f32),
            scratch_shapes=scratch,
            compiler_params=params(56 if streamed else 6),
            name="interact",
        )(index, *rows, *bases, blocks)

    row = struct((LEAF, width), bf16)
    payload = struct((3, LEAF, TILE), bf16)
    pairs = width // TILE

    rows_b, rows_a = node_halo(probes)
    coords, pay, rows, basis, transfer = pl.pallas_call(
        coords_kernel,
        in_specs=[SMEM, VMEM, HBM, HBM, HBM],
        out_specs=(VMEM,) * 5,
        out_shape=(row, payload, row, row, row),
        scratch_shapes=[pltpu.SemaphoreType.DMA((3, STEPS // 2))],
        compiler_params=params(56),
        name="coords",
    )(scal, inner_tree, probes, inner_basis, inner_transfer)
    mine = coarse_near(pay, node)
    mine, near_table, far_table = lax.optimization_barrier((mine, near_table, far_table))
    other = swap(mine, 6)
    coords_b, coords_a = node_halo(after(coords, mine))
    basis_b, basis_a = node_halo(after(outer_basis, mine))
    near_part = interact(near_table, (rows_b, after(rows, mine), rows_a), inner_near, streamed=STREAM[0])
    other, near_part = lax.optimization_barrier((other, near_part))
    one = adjacent_rows(far_payload(mine, other, node))
    far_part = interact(far_table, (coords_b, coords, coords_a), inner_far, streamed=STREAM[1])
    far_part, basis_b, basis_a = lax.optimization_barrier((far_part, basis_b, basis_a))
    one, far_part = lax.optimization_barrier((one, far_part))
    two = swap(one, 1)
    middle = pl.pallas_call(
        inner_kernel,
        in_specs=[SMEM] + [VMEM] * 10,
        out_specs=VMEM,
        out_shape=row,
        scratch_shapes=[pltpu.VMEM((LEAF, width), bf16)],
        compiler_params=params(6),
        name="inner",
    )(scal, near_part, far_part, basis, transfer, mine, other, one, two, inner_tree, inner_links)
    middle_b, middle_a = node_halo(middle)
    coords, pay = pl.pallas_call(
        next_kernel,
        in_specs=[SMEM] + [VMEM] * 4,
        out_specs=(VMEM, VMEM),
        out_shape=(row, payload),
        compiler_params=params(6),
        name="next",
    )(scal, outer_tree, after(middle, middle_a), outer_basis, outer_transfer)
    mine = coarse_near(pay, node)
    other = swap(mine, 6)
    near_part = interact(near_table, (middle_b, after(middle, mine), middle_a), outer_near)
    other, near_part = lax.optimization_barrier((other, near_part))
    one = adjacent_rows(far_payload(mine, other, node))
    far_part = interact(far_table, (middle_b, coords, middle_a), outer_far, (basis_b, basis_a))
    one, far_part = lax.optimization_barrier((one, far_part))
    two = swap(one, 1)
    samples, grams, gram = pl.pallas_call(
        outer_kernel,
        in_specs=[SMEM] + [VMEM] * 10,
        out_specs=(VMEM,) * 3,
        out_shape=(
            struct((LEAF, width), f32),
            struct((pairs // 2, LEAF, TILE), f32),
            struct((LEAF, TILE), f32),
        ),
        scratch_shapes=[pltpu.VMEM((LEAF, width), bf16)],
        compiler_params=params(6),
        name="outer",
    )(scal, near_part, far_part, outer_basis, outer_transfer, mine, other, one, two, outer_tree, outer_links)
    def piece(n, work):
        return pl.pallas_call(
            lambda *refs: pair_kernel(*refs, first=2 * n, last=2 * n + 2),
            in_specs=[VMEM],
            out_specs=VMEM,
            out_shape=struct(work.shape, f32),
            scratch_shapes=elimination(pairs // 2),
            input_output_aliases={0: 0},
            compiler_params=params(6),
            name="pairs",
        )(work)

    work = grams
    for n, mask in enumerate((1, 2, 6, 8)):
        other = swap(gram, mask)
        work = piece(n, work)
        gram, work = lax.optimization_barrier((gram + other, work))
    other = swap(gram, 24)
    pair_basis = pl.pallas_call(
        solve_kernel,
        in_specs=[VMEM, VMEM],
        out_specs=VMEM,
        out_shape=struct((LEAF, width), f32),
        compiler_params=params(6),
        name="solve",
    )(work, samples)
    gram = gram + other
    scale = pairs * lax.axis_size("leaf")
    group_basis = pl.pallas_call(
        lambda *refs: group_kernel(*refs, scale=scale),
        in_specs=[VMEM, VMEM],
        out_specs=VMEM,
        out_shape=struct((LEAF, pairs * LEAF), f32),
        scratch_shapes=[pltpu.VMEM((1, LEAF, TILE), f32)],
        compiler_params=params(6),
        name="group",
    )(gram, work)
    return (pair_basis, group_basis)


def solution(mesh):
    flat = P(None, AXES)
    index = P(AXES, None)
    blocks = P(None, None, AXES)
    tree = P(None, None, None, AXES)
    factor = (blocks, flat, blocks, flat, tree, tree)
    return jax.shard_map(
        local,
        mesh=mesh,
        in_specs=(flat, index, index) + factor + factor,
        out_specs=(flat, flat),
        check_vma=False,
    )
```

```python
import jax
import jax.numpy as jnp
from jax import lax
from jax.experimental import pallas as pl
from jax.experimental.pallas import tpu as pltpu
from jax.sharding import PartitionSpec as P


AXES = ("box", "leaf")
LEAF = 64
TILE = 128
STEPS = 8
STREAM = (False, False)
bf16 = jnp.bfloat16
f32 = jnp.float32

NN = (((1,), (0,)), ((), ()))
NT = (((1,), (1,)), ((), ()))


def dot(a, b, dims=NN, precision=None):
    return lax.dot_general(a, b, dims, precision=precision, preferred_element_type=f32)


def low_half(shape):
    return lax.broadcasted_iota(jnp.int32, shape, len(shape) - 1) < LEAF


def two_blocks(tile):
    low = low_half(tile.shape)
    zero = jnp.zeros_like(tile)
    return jnp.concatenate([jnp.where(low, tile, zero), jnp.where(low, zero, tile)], axis=0)


def swap_halves(tile):
    return jnp.concatenate([tile[:, LEAF:], tile[:, :LEAF]], axis=1)


def twice(block):
    return jnp.concatenate([block, block], axis=1)


def lanes(t):
    return pl.ds(pl.multiple_of(t * TILE, TILE), TILE)


def coarse_payload(sums, tree_ref, scal_ref, pay_ref):
    folded = sums + swap_halves(sums)
    pay_ref[0] = folded.astype(bf16)
    up = dot(folded[:, :LEAF].astype(bf16), tree_ref[0, scal_ref[0] % 2])
    pay_ref[1] = twice(up).astype(bf16)
    up = dot(up.astype(bf16), tree_ref[1, scal_ref[0] // 2 % 2])
    pay_ref[2] = twice(up).astype(bf16)


def split(x):
    high = x.astype(bf16)
    return high, (x - high.astype(f32)).astype(bf16)


def dot3(a, b, dims=NN):
    ah, al = split(a)
    bh, bl = split(b)
    side = dims[0][1][0]
    return dot(jnp.concatenate([ah, ah, al], axis=1), jnp.concatenate([bh, bl, bh], axis=side), dims)


def fetch(sources, targets, sems, chunks):
    def piece(n, g):
        source, target = sources[n], targets[n]
        wide = source.shape[-1] // chunks
        at = (slice(None),) * (len(source.shape) - 1) + (pl.ds(g * wide, wide),)
        return pltpu.make_async_copy(source.at[at], target.at[at], sems.at[n, g])

    for g in range(chunks):
        for n in range(len(sources)):
            piece(n, g).start()

    def wait(g):
        for n in range(len(sources)):
            piece(n, g).wait()

    return wait


def coords_kernel(scal_ref, tree_hbm, probes_hbm, basis_hbm, transfer_hbm, coords_ref, pay_ref, rows_ref, basis_ref, transfer_ref, tree_ref, sems, tree_sem):
    tree = pltpu.make_async_copy(tree_hbm, tree_ref, tree_sem)
    wait = fetch((probes_hbm, basis_hbm, transfer_hbm), (rows_ref, basis_ref, transfer_ref), sems, STEPS // 2)
    tree.start()
    per = rows_ref.shape[1] // TILE // (STEPS // 2)
    for g in range(STEPS // 2):
        wait(g)
        for u in range(per):
            at = slice((g * per + u) * TILE, (g * per + u + 1) * TILE)
            coords_ref[:, at] = dot(rows_ref[:, at], two_blocks(basis_ref[:, at]), NT).astype(bf16)
    tree.wait()
    coarse_payload(node_sums(coords_ref, transfer_ref), tree_ref, scal_ref, pay_ref)


def node_sums(coords_ref, transfer_ref):
    def step(g, sums):
        for u in range(16):
            at = lanes(g * 16 + u)
            sums = sums + dot(coords_ref[:, at], two_blocks(transfer_ref[:, at]))
        return sums

    return lax.fori_loop(0, coords_ref.shape[1] // TILE // 16, step, jnp.zeros((LEAF, TILE), f32))


def by_tiles(count, one):
    def step(g, carry):
        for u in range(16):
            one(lanes(g * 16 + u))
        return carry

    lax.fori_loop(0, count // 16, step, 0)


def store_tile(store_ref, t, tile):
    store_ref[t] = tile
    store_ref[store_ref.shape[0] // 2 + t] = swap_halves(tile)


def fill_store(store_ref, sources, bases):
    tiles = sources[0].shape[1] // TILE
    for n, (source, basis) in enumerate(zip(sources, bases)):

        def step(g, carry, n=n, source=source, basis=basis):
            for u in range(16):
                t = g * 16 + u
                tile = source[:, lanes(t)]
                if basis is not None:
                    tile = dot(tile, two_blocks(basis[:, lanes(t)]), NT).astype(bf16)
                store_tile(store_ref, n * tiles + t, tile)
            return carry

        lax.fori_loop(0, tiles // 16, step, 0)


def gathered(store_ref, index_ref, pair, low):
    rows = []
    for h in range(2):
        base = (2 * pair + h) * 8
        cols = []
        for k in range(4):
            first = store_ref[index_ref[base + 2 * k]]
            second = store_ref[index_ref[base + 2 * k + 1]]
            cols.append(jnp.where(low, first, second))
        rows.append(jnp.concatenate(cols, axis=1))
    return jnp.concatenate(rows, axis=0)


def interact_kernel(index_ref, before_ref, own_ref, after_ref, *refs, streamed):
    if streamed:
        *bases, blocks_hbm, out_ref, store_ref, blocks_ref, sems = refs
        wide = blocks_ref.shape[2] // STEPS

        def piece(g):
            at = (slice(None), slice(None), pl.ds(pl.multiple_of(g * wide, wide), wide))
            return pltpu.make_async_copy(blocks_hbm.at[at], blocks_ref.at[at], sems.at[g])

        for g in range(STEPS):
            piece(g).start()
    else:
        *bases, blocks_ref, out_ref, store_ref = refs
    bases = (bases[0], None, bases[1]) if bases else (None, None, None)
    fill_store(store_ref, (before_ref, own_ref, after_ref), bases)
    low = low_half((LEAF, TILE))
    steps = STEPS if streamed else STEPS // 4
    per = own_ref.shape[1] // TILE // steps

    def step(g, carry):
        if streamed:
            piece(g).wait()
        for u in range(per):
            pair = g * per + u
            blocks = blocks_ref[:, :, lanes(pair)].reshape(8 * LEAF, TILE)
            both = dot(gathered(store_ref, index_ref, pair, low), blocks)
            out_ref[:, lanes(pair)] = jnp.where(low, both[:LEAF], both[LEAF:])
        return carry

    lax.fori_loop(0, steps, step, 0)


def descend(scal_ref, mine_ref, other_ref, first_ref, second_ref, tree_ref, links_ref, blocks):
    node = scal_ref[0]
    b0, b1, b2 = node % 2, node // 2 % 2, node // 4 % 2
    block = node // 8
    odd, has_left, has_right = block % 2, block > 0, block < blocks - 1

    def low_group(n):
        return jnp.where(b2 == 0, mine_ref[n], other_ref[n])

    def high_group(n):
        return jnp.where(b2 == 0, other_ref[n], mine_ref[n])

    crossed = (odd == 1) == (b0 == 0)

    def left(n):
        tile = jnp.where(crossed, first_ref[n], second_ref[n])
        return jnp.where(has_left, tile, jnp.zeros_like(tile))

    def right(n):
        tile = jnp.where(crossed, second_ref[n], first_ref[n])
        return jnp.where(has_right, tile, jnp.zeros_like(tile))

    def pick(j, options):
        tile = options[-1]
        for n in range(len(options) - 2, -1, -1):
            tile = jnp.where(j == n, options[n], tile)
        return tile

    ext0 = [left(2), low_group(0), low_group(1), high_group(0), high_group(1), right(2)]
    ext1 = [left(1), low_group(2), high_group(2), right(1)]
    j0, j1 = b2 * 2 + b1, b2
    around = [
        (pick(j0, ext0[:4]), pick(j0, ext0[2:])),
        (pick(j1, ext1[:2]), pick(j1, ext1[2:])),
        (left(0), right(0)),
    ]
    coupled = []
    for c, parity in enumerate((b0, b1, b2)):
        mid = links_ref[c, 1]
        none = jnp.zeros_like(mid)
        lo = jnp.concatenate([links_ref[c, 0], jnp.where(parity == 1, mid, none)], axis=0)
        hi = jnp.concatenate([jnp.where(parity == 0, mid, none), links_ref[c, 2]], axis=0)
        coupled.append(dot(around[c][0], lo) + dot(around[c][1], hi))
    h = coupled[1] + dot(coupled[2].astype(bf16), tree_ref[1, b1], NT)
    h = coupled[0] + dot(h.astype(bf16), tree_ref[0, b0], NT)
    return twice(h).astype(bf16)


def finish(near_ref, far_ref, basis_ref, transfer_ref, descent, coeffs_ref, out_ref):
    def coeffs(at):
        down = dot(descent, two_blocks(transfer_ref[:, at]), NT)
        coeffs_ref[:, at] = (far_ref[:, at] + down).astype(bf16)

    def result(at):
        out = near_ref[:, at] + dot(coeffs_ref[:, at], two_blocks(basis_ref[:, at]))
        out_ref[:, at] = out.astype(out_ref.dtype)

    count = near_ref.shape[1] // TILE
    by_tiles(count, coeffs)
    by_tiles(count, result)


def inner_kernel(
    scal_ref, near_ref, far_ref, basis_ref, transfer_ref,
    mine_ref, other_ref, first_ref, second_ref, tree_ref, links_ref,
    middle_ref, coeffs_ref, *, blocks,
):
    descent = descend(scal_ref, mine_ref, other_ref, first_ref, second_ref, tree_ref, links_ref, blocks)
    finish(near_ref, far_ref, basis_ref, transfer_ref, descent, coeffs_ref, middle_ref)


def next_kernel(scal_ref, tree_ref, rows_ref, basis_ref, transfer_ref, coords_ref, pay_ref):
    def coords(at):
        coords_ref[:, at] = dot(rows_ref[:, at], two_blocks(basis_ref[:, at]), NT).astype(bf16)

    by_tiles(rows_ref.shape[1] // TILE, coords)
    coarse_payload(node_sums(coords_ref, transfer_ref), tree_ref, scal_ref, pay_ref)


def outer_kernel(
    scal_ref, near_ref, far_ref, basis_ref, transfer_ref,
    mine_ref, other_ref, first_ref, second_ref, tree_ref, links_ref,
    samples_ref, work_ref, gram_ref, coeffs_ref, *, blocks,
):
    descent = descend(scal_ref, mine_ref, other_ref, first_ref, second_ref, tree_ref, links_ref, blocks)
    finish(near_ref, far_ref, basis_ref, transfer_ref, descent, coeffs_ref, samples_ref)
    low = low_half((LEAF, TILE))

    def step(g, total):
        for u in range(8):
            t = g * 8 + u
            both = jnp.concatenate([samples_ref[:, lanes(2 * t)], samples_ref[:, lanes(2 * t + 1)]], axis=0)
            both = dot3(both, both, NT)
            gram = jnp.where(low, both[:LEAF], both[LEAF:]) / TILE
            work_ref[t] = gram
            total = total + gram
        return total

    total = lax.fori_loop(0, work_ref.shape[0] // 8, step, jnp.zeros((LEAF, TILE), f32))
    gram_ref[...] = total + swap_halves(total)


def lane_take(tile, index):
    return jnp.take_along_axis(tile, index, axis=1, mode="promise_in_bounds")


def each(count, unroll, one):
    unroll = min(unroll, count)

    def step(g, carry):
        for u in range(unroll):
            one(g * unroll + u)
        return carry

    lax.fori_loop(0, count // unroll, step, 0)


def eliminate(work_ref, tee_ref, first=0, last=LEAF // 8):
    count = work_ref.shape[0]
    per = min(count, 4)
    groups = count // per
    sub = lax.broadcasted_iota(jnp.int32, (8, TILE), 0)
    lane = lax.broadcasted_iota(jnp.int32, (8, TILE), 1)
    col, half = lane % LEAF, lane // LEAF
    panels = LEAF // 8
    for kb in range(first, last):
        base = kb * 8
        rows = slice(base, base + 8)
        inside = (col >= base) & (col < base + 8)
        cols = []
        for g in range(groups):
            tiles = [work_ref[g * per + t, rows, :] for t in range(per)]
            packed = []
            for j in range(8):
                index = lane // 16 % 2 * LEAF + (base + j)
                value = lane_take(tiles[0], index)
                for t in range(1, per):
                    value = jnp.where(lane // 32 == t, lane_take(tiles[t], index), value)
                packed.append(value)
            cols.append(packed)
        tees = [[] for _ in range(groups)]
        for j in range(8):
            for c, tee in zip(cols, tees):
                inv = lax.rsqrt(c[j][j : j + 1, :])
                lower = c[j] * inv
                below = jnp.where(sub > j, lower, 0.0)
                for n in range(j + 1, 8):
                    c[n] = c[n] - lower * lower[n : n + 1, :]
                for n in range(j):
                    row = tee[n][j : j + 1, :] * inv
                    tee[n] = jnp.where(sub == j, row, tee[n] - below * row)
                tee.append(jnp.where(sub == j, inv, -below * inv))
        for g in range(groups):
            for j in range(8):
                tee_ref[g * 8 + j] = tees[g][j]

        for tt in range(per):
            index = tt * 32 + half * 16
            for g in range(groups):
                t = g * per + tt
                panel = work_ref[t, rows, :]
                spread = [lane_take(tee_ref[g * 8 + j], index) for j in range(8)]
                done = spread[0] * panel[:1, :]
                for j in range(1, 8):
                    done = done + spread[j] * panel[j : j + 1, :]
                for j in range(8):
                    done = jnp.where((col == base + j) & (sub >= j), spread[j], done)
                work_ref[t, rows, :] = done
        if kb == panels - 1:
            break

        rest_rows = LEAF - base - 8

        def update(t):
            left = work_ref[t, rows, :]
            right = jnp.where(inside & (col > base + sub), 0.0, left)
            turned = stacked(left, (0, 0, 1)).T.astype(bf16)
            turned = jnp.concatenate([turned[base + 8 : LEAF], turned[LEAF + base + 8 :]], axis=0)
            both = dot(turned, stacked(right, (0, 1, 0)).astype(bf16))
            for ib in range(kb + 1, panels):
                at = slice(ib * 8, ib * 8 + 8)
                n = (ib - kb - 1) * 8
                rest = jnp.where(inside, 0.0, work_ref[t, at, :])
                work_ref[t, at, :] = rest - jnp.where(half == 0, both[n : n + 8], both[rest_rows + n : rest_rows + n + 8])

        each(count, 16, update)


def stacked(x, order):
    high = x.astype(bf16).astype(f32)
    pieces = (high, x - high)
    return jnp.concatenate([pieces[n] for n in order] + [jnp.zeros_like(x)], axis=0)


def parts(tile):
    row = lax.broadcasted_iota(jnp.int32, tile.shape, 0)
    col = lax.broadcasted_iota(jnp.int32, tile.shape, 1) % LEAF
    return row, col


def pair_kernel(before_ref, work_ref, tee_ref, *, first, last):
    work_ref[...] = before_ref[...]
    eliminate(work_ref, tee_ref, first, last)


def solve_kernel(work_ref, samples_ref, basis_ref):
    def solve(t):
        tile = work_ref[t]
        row, col = parts(tile)
        inverse = two_blocks(jnp.where(col <= row, tile, 0.0))
        one, two = lanes(2 * t), lanes(2 * t + 1)
        solved = dot3(inverse, jnp.concatenate([samples_ref[:, one], samples_ref[:, two]], axis=0))
        basis_ref[:, one] = solved[:LEAF]
        basis_ref[:, two] = solved[LEAF:]

    each(work_ref.shape[0], 8, solve)


def eliminate_few(load, save, count):
    shape = (count, 8, TILE)
    sub = lax.broadcasted_iota(jnp.int32, shape, 1)
    lane = lax.broadcasted_iota(jnp.int32, shape, 2)
    low = lane < LEAF
    col = lane % LEAF
    panels = LEAF // 8
    for kb in range(panels):
        panel = load(kb)
        cols = []
        for j in range(8):
            k = kb * 8 + j
            one = jnp.broadcast_to(panel[:, :, k : k + 1], shape)
            two = jnp.broadcast_to(panel[:, :, LEAF + k : LEAF + k + 1], shape)
            cols.append(jnp.where(low, one, two))
        rows = []
        for j in range(8):
            k = kb * 8 + j
            inv = lax.rsqrt(cols[j][:, j : j + 1, :])
            lower = cols[j] * inv
            for n in range(j + 1, 8):
                cols[n] = cols[n] - lower * lower[:, n : n + 1, :]
            row = jnp.where(col[:, :1] == k, inv, panel[:, j : j + 1, :] * inv)
            below = sub > j
            kept = jnp.where(below & (col == k), 0.0, panel)
            panel = jnp.where(sub == j, row, kept - jnp.where(below, lower, 0.0) * row)
            rows.append(row)
        save(kb, panel)
        if kb == panels - 1:
            break
        turned = jnp.swapaxes(panel, 1, 2)
        inside = (col >= kb * 8) & (col < kb * 8 + 8)
        for j in range(8):
            k = kb * 8 + j
            rows[j] = jnp.where((col[:, :1] > k) & (col[:, :1] < kb * 8 + 8), 0.0, rows[j])
        for ib in range(kb + 1, panels):
            rest = jnp.where(inside, 0.0, load(ib))
            for j in range(8):
                one = jnp.broadcast_to(turned[:, ib * 8 : ib * 8 + 8, j : j + 1], shape)
                two = jnp.broadcast_to(turned[:, LEAF + ib * 8 : LEAF + ib * 8 + 8, j : j + 1], shape)
                rest = rest - jnp.where(low, one, two) * rows[j]
            save(ib, rest)


def group_kernel(gram_ref, work_ref, out_ref, own_ref, *, scale):
    own_ref[0] = gram_ref[...] / scale

    def load(b):
        return own_ref[:, b * 8 : b * 8 + 8, :]

    def save(b, value):
        own_ref[:, b * 8 : b * 8 + 8, :] = value

    eliminate_few(load, save, 1)
    tile = own_ref[0]
    row, col = parts(tile)
    inverse = jnp.where(col <= row, tile, 0.0)

    def solve(t):
        tile = work_ref[t]
        upper = jnp.where(col > row, tile, jnp.where(col == row, 1.0 / tile, 0.0))
        out_ref[:, lanes(t)] = dot3(inverse, two_blocks(upper), NT)

    each(work_ref.shape[0], 8, solve)


HBM = pl.BlockSpec(memory_space=pltpu.HBM)
VMEM = pl.BlockSpec(memory_space=pltpu.VMEM)
SMEM = pl.BlockSpec(memory_space=pltpu.SMEM)


def params(mib):
    return pltpu.CompilerParams(vmem_limit_bytes=mib * 2**20)


def elimination(count):
    return [
        pltpu.VMEM((max(count // 4, 1) * 8, 8, TILE), f32),
    ]


def struct(shape, dtype):
    return jax.ShapeDtypeStruct(shape, dtype)


def swap(x, mask):
    count = lax.axis_size(AXES)
    return lax.ppermute(x, AXES, [(i, i ^ mask) for i in range(count)])


def adjacent_rows(x):
    count = lax.axis_size(AXES)
    route = []
    for i in range(count):
        forward = (i // 8 % 2 == 0) == (i % 2 == 0)
        route.append((i, (i + 8 if forward else i - 8) % count))
    return lax.ppermute(x, AXES, route)


def node_halo(x):
    count = lax.axis_size(AXES)
    route = [(i, (i - 1 if i % 2 == 0 else i + 1) % count) for i in range(count)]
    far = lax.ppermute(x, AXES, route)
    near = swap(x, 1)
    return far, near


def leaf_table(index, node):
    leaves = index.shape[0]
    place = index - (node - 1) * leaves
    block = place // leaves
    block = jnp.where(node % 2 == 1, 2 - block, block)
    place = block * leaves + place % leaves
    slot = lax.broadcasted_iota(jnp.int32, index.shape, 1)
    return (((place + slot) % 2) * (3 * leaves // 2) + place // 2).reshape(-1)


def coarse_near(pay, node):
    low = low_half((LEAF, TILE))
    b0, b1 = node % 2, node // 2 % 2

    def halves(bit, mine, other):
        return jnp.where(low == (bit == 0), mine, other)

    other = swap(pay, 1)
    z0 = halves(b0, pay[0], other[0])
    stage = jnp.stack([z0, pay[1] + other[1], pay[2] + other[2]])
    other = swap(stage, 2)
    first = jnp.where(b1 == 0, stage[0], other[0])
    second = jnp.where(b1 == 0, other[0], stage[0])
    return jnp.stack([first, second, halves(b1, stage[1], other[1]), stage[2] + other[2]])


def far_payload(mine, other, node):
    low = low_half((LEAF, TILE))
    b2, odd = node // 4 % 2, node // 8 % 2
    top = jnp.where(low == (b2 == 0), mine[3], other[3])
    lo = jnp.where(b2 == 0, mine, other)
    hi = jnp.where(b2 == 0, other, mine)
    rightward = jnp.stack([top, hi[2], hi[1]])
    leftward = jnp.stack([top, lo[2], lo[0]])
    return jnp.where((odd == 0) == (node % 2 == 0), rightward, leftward)


def after(x, *values):
    return lax.optimization_barrier((x, *values))[0]


def local(
    probes,
    near_index,
    far_index,
    inner_near,
    inner_basis,
    inner_far,
    inner_transfer,
    inner_tree,
    inner_links,
    outer_near,
    outer_basis,
    outer_far,
    outer_transfer,
    outer_tree,
    outer_links,
):
    node = lax.axis_index(AXES)
    count = lax.axis_size(AXES)
    width = probes.shape[1]
    scal = node.reshape(1).astype(jnp.int32)
    near_table = leaf_table(near_index, node)
    far_table = leaf_table(far_index, node)

    def interact(index, rows, blocks, bases=(), streamed=False):
        scratch = [pltpu.VMEM((3 * width // LEAF, LEAF, TILE), bf16)]
        if streamed:
            scratch += [pltpu.VMEM(blocks.shape, bf16), pltpu.SemaphoreType.DMA((STEPS,))]
        return pl.pallas_call(
            lambda *refs: interact_kernel(*refs, streamed=streamed),
            in_specs=[SMEM] + [VMEM] * (3 + len(bases)) + [HBM if streamed else VMEM],
            out_specs=VMEM,
            out_shape=struct((LEAF, width), f32),
            scratch_shapes=scratch,
            compiler_params=params(56 if streamed else 6),
            name="interact",
        )(index, *rows, *bases, blocks)

    row = struct((LEAF, width), bf16)
    payload = struct((3, LEAF, TILE), bf16)
    pairs = width // TILE

    rows_b, rows_a = node_halo(probes)
    coords, pay, rows, basis, transfer = pl.pallas_call(
        coords_kernel,
        in_specs=[SMEM, HBM, HBM, HBM, HBM],
        out_specs=(VMEM,) * 5,
        out_shape=(row, payload, row, row, row),
        scratch_shapes=[
            pltpu.VMEM(inner_tree.shape, bf16),
            pltpu.SemaphoreType.DMA((3, STEPS // 2)),
            pltpu.SemaphoreType.DMA,
        ],
        compiler_params=params(52),
        name="coords",
    )(scal, inner_tree, probes, inner_basis, inner_transfer)
    mine = coarse_near(pay, node)
    mine, near_table, far_table = lax.optimization_barrier((mine, near_table, far_table))
    other = swap(mine, 6)
    coords_b, coords_a = node_halo(after(coords, mine))
    near_part = interact(near_table, (rows_b, after(rows, mine), rows_a), inner_near, streamed=STREAM[0])
    other, near_part = lax.optimization_barrier((other, near_part))
    one = adjacent_rows(far_payload(mine, other, node))
    basis_b, basis_a = node_halo(after(outer_basis, near_part))
    far_part = interact(far_table, (coords_b, coords, coords_a), inner_far, streamed=STREAM[1])
    one, far_part = lax.optimization_barrier((one, far_part))
    two = swap(one, 1)
    middle = pl.pallas_call(
        lambda *refs: inner_kernel(*refs, blocks=count // 8),
        in_specs=[SMEM] + [VMEM] * 10,
        out_specs=VMEM,
        out_shape=row,
        scratch_shapes=[pltpu.VMEM((LEAF, width), bf16)],
        compiler_params=params(6),
        name="inner",
    )(scal, near_part, far_part, basis, transfer, mine, other, one, two, inner_tree, inner_links)
    middle_b, middle_a = node_halo(middle)
    coords, pay = pl.pallas_call(
        next_kernel,
        in_specs=[SMEM] + [VMEM] * 4,
        out_specs=(VMEM, VMEM),
        out_shape=(row, payload),
        compiler_params=params(6),
        name="next",
    )(scal, outer_tree, after(middle, middle_a), outer_basis, outer_transfer)
    mine = coarse_near(pay, node)
    other = swap(mine, 6)
    near_part = interact(near_table, (middle_b, after(middle, mine), middle_a), outer_near)
    other, near_part = lax.optimization_barrier((other, near_part))
    one = adjacent_rows(far_payload(mine, other, node))
    far_part = interact(far_table, (middle_b, coords, middle_a), outer_far, (basis_b, basis_a))
    one, far_part = lax.optimization_barrier((one, far_part))
    two = swap(one, 1)
    samples, grams, gram = pl.pallas_call(
        lambda *refs: outer_kernel(*refs, blocks=count // 8),
        in_specs=[SMEM] + [VMEM] * 10,
        out_specs=(VMEM,) * 3,
        out_shape=(
            struct((LEAF, width), f32),
            struct((pairs // 2, LEAF, TILE), f32),
            struct((LEAF, TILE), f32),
        ),
        scratch_shapes=[pltpu.VMEM((LEAF, width), bf16)],
        compiler_params=params(6),
        name="outer",
    )(scal, near_part, far_part, outer_basis, outer_transfer, mine, other, one, two, outer_tree, outer_links)

    def piece(n, work):
        return pl.pallas_call(
            lambda *refs: pair_kernel(*refs, first=2 * n, last=2 * n + 2),
            in_specs=[VMEM],
            out_specs=VMEM,
            out_shape=struct(work.shape, f32),
            scratch_shapes=elimination(pairs // 2),
            input_output_aliases={0: 0},
            compiler_params=params(6),
            name="pairs",
        )(work)

    work = grams
    for n, mask in enumerate((1, 2, 6, 8)):
        other = swap(gram, mask)
        work = piece(n, work)
        gram, work = lax.optimization_barrier((gram + other, work))
    other = swap(gram, 24)
    pair_basis = pl.pallas_call(
        solve_kernel,
        in_specs=[VMEM, VMEM],
        out_specs=VMEM,
        out_shape=struct((LEAF, width), f32),
        compiler_params=params(6),
        name="solve",
    )(work, samples)
    gram = gram + other
    scale = pairs * lax.axis_size("leaf")
    group_basis = pl.pallas_call(
        lambda *refs: group_kernel(*refs, scale=scale),
        in_specs=[VMEM, VMEM],
        out_specs=VMEM,
        out_shape=struct((LEAF, pairs * LEAF), f32),
        scratch_shapes=[pltpu.VMEM((1, LEAF, TILE), f32)],
        compiler_params=params(6),
        name="group",
    )(gram, work)
    return (pair_basis, group_basis)


def solution(mesh):
    flat = P(None, AXES)
    index = P(AXES, None)
    blocks = P(None, None, AXES)
    tree = P(None, None, None, AXES)
    factor = (blocks, flat, blocks, flat, tree, tree)
    return jax.shard_map(
        local,
        mesh=mesh,
        in_specs=(flat, index, index) + factor + factor,
        out_specs=(flat, flat),
        check_vma=False,
    )
```

```python
import jax
import jax.numpy as jnp
from jax import lax
from jax.experimental import pallas as pl
from jax.experimental.pallas import tpu as pltpu
from jax.sharding import PartitionSpec as P


AXES = ("box", "leaf")
LEAF = 64
TILE = 128
STEPS = 8
STREAM = (False, False)
bf16 = jnp.bfloat16
f32 = jnp.float32

NN = (((1,), (0,)), ((), ()))
NT = (((1,), (1,)), ((), ()))


def dot(a, b, dims=NN, precision=None):
    return lax.dot_general(a, b, dims, precision=precision, preferred_element_type=f32)


def low_half(shape):
    return lax.broadcasted_iota(jnp.int32, shape, len(shape) - 1) < LEAF


def two_blocks(tile):
    low = low_half(tile.shape)
    zero = jnp.zeros_like(tile)
    return jnp.concatenate([jnp.where(low, tile, zero), jnp.where(low, zero, tile)], axis=0)


def swap_halves(tile):
    return jnp.concatenate([tile[:, LEAF:], tile[:, :LEAF]], axis=1)


def twice(block):
    return jnp.concatenate([block, block], axis=1)


def lanes(t):
    return pl.ds(pl.multiple_of(t * TILE, TILE), TILE)


def coarse_payload(sums, tree_ref, scal_ref, pay_ref):
    folded = sums + swap_halves(sums)
    pay_ref[0] = folded.astype(bf16)
    up = dot(folded[:, :LEAF].astype(bf16), tree_ref[0, scal_ref[0] % 2])
    pay_ref[1] = twice(up).astype(bf16)
    up = dot(up.astype(bf16), tree_ref[1, scal_ref[0] // 2 % 2])
    pay_ref[2] = twice(up).astype(bf16)


def split(x):
    high = x.astype(bf16)
    return high, (x - high.astype(f32)).astype(bf16)


def dot3(a, b, dims=NN):
    ah, al = split(a)
    bh, bl = split(b)
    side = dims[0][1][0]
    return dot(jnp.concatenate([ah, ah, al], axis=1), jnp.concatenate([bh, bl, bh], axis=side), dims)


def fetch(sources, targets, sems, chunks):
    def piece(n, g):
        source, target = sources[n], targets[n]
        wide = source.shape[-1] // chunks
        at = (slice(None),) * (len(source.shape) - 1) + (pl.ds(g * wide, wide),)
        return pltpu.make_async_copy(source.at[at], target.at[at], sems.at[n, g])

    for g in range(chunks):
        for n in range(len(sources)):
            piece(n, g).start()

    def wait(g):
        for n in range(len(sources)):
            piece(n, g).wait()

    return wait


def coords_kernel(scal_ref, tree_hbm, probes_hbm, basis_hbm, transfer_hbm, coords_ref, pay_ref, rows_ref, basis_ref, transfer_ref, tree_ref, sems, tree_sem):
    tree = pltpu.make_async_copy(tree_hbm, tree_ref, tree_sem)
    wait = fetch((probes_hbm, basis_hbm, transfer_hbm), (rows_ref, basis_ref, transfer_ref), sems, STEPS // 2)
    tree.start()
    per = rows_ref.shape[1] // TILE // (STEPS // 2)
    for g in range(STEPS // 2):
        wait(g)
        for u in range(per):
            at = slice((g * per + u) * TILE, (g * per + u + 1) * TILE)
            coords_ref[:, at] = dot(rows_ref[:, at], two_blocks(basis_ref[:, at]), NT).astype(bf16)
    tree.wait()
    coarse_payload(node_sums(coords_ref, transfer_ref), tree_ref, scal_ref, pay_ref)


def node_sums(coords_ref, transfer_ref):
    def step(g, sums):
        for u in range(16):
            at = lanes(g * 16 + u)
            sums = sums + dot(coords_ref[:, at], two_blocks(transfer_ref[:, at]))
        return sums

    return lax.fori_loop(0, coords_ref.shape[1] // TILE // 16, step, jnp.zeros((LEAF, TILE), f32))


def by_tiles(count, one):
    def step(g, carry):
        for u in range(16):
            one(lanes(g * 16 + u))
        return carry

    lax.fori_loop(0, count // 16, step, 0)


def store_tile(store_ref, t, tile):
    store_ref[t] = tile
    store_ref[store_ref.shape[0] // 2 + t] = swap_halves(tile)


def fill_store(store_ref, sources, bases):
    tiles = sources[0].shape[1] // TILE
    for n, (source, basis) in enumerate(zip(sources, bases)):

        def step(g, carry, n=n, source=source, basis=basis):
            for u in range(16):
                t = g * 16 + u
                tile = source[:, lanes(t)]
                if basis is not None:
                    tile = dot(tile, two_blocks(basis[:, lanes(t)]), NT).astype(bf16)
                store_tile(store_ref, n * tiles + t, tile)
            return carry

        lax.fori_loop(0, tiles // 16, step, 0)


def gathered(store_ref, index_ref, pair, low):
    rows = []
    for h in range(2):
        base = (2 * pair + h) * 8
        cols = []
        for k in range(4):
            first = store_ref[index_ref[base + 2 * k]]
            second = store_ref[index_ref[base + 2 * k + 1]]
            cols.append(jnp.where(low, first, second))
        rows.append(jnp.concatenate(cols, axis=1))
    return jnp.concatenate(rows, axis=0)


def interact_kernel(index_ref, before_ref, own_ref, after_ref, *refs, streamed):
    if streamed:
        *bases, blocks_hbm, out_ref, store_ref, blocks_ref, sems = refs
        wide = blocks_ref.shape[2] // STEPS

        def piece(g):
            at = (slice(None), slice(None), pl.ds(pl.multiple_of(g * wide, wide), wide))
            return pltpu.make_async_copy(blocks_hbm.at[at], blocks_ref.at[at], sems.at[g])

        for g in range(STEPS):
            piece(g).start()
    else:
        *bases, blocks_ref, out_ref, store_ref = refs
    bases = (bases[0], None, bases[1]) if bases else (None, None, None)
    fill_store(store_ref, (before_ref, own_ref, after_ref), bases)
    low = low_half((LEAF, TILE))
    steps = STEPS if streamed else STEPS // 4
    per = own_ref.shape[1] // TILE // steps

    def step(g, carry):
        if streamed:
            piece(g).wait()
        for u in range(per):
            pair = g * per + u
            blocks = blocks_ref[:, :, lanes(pair)].reshape(8 * LEAF, TILE)
            both = dot(gathered(store_ref, index_ref, pair, low), blocks)
            out_ref[:, lanes(pair)] = jnp.where(low, both[:LEAF], both[LEAF:])
        return carry

    lax.fori_loop(0, steps, step, 0)


def descend(scal_ref, mine_ref, other_ref, first_ref, second_ref, tree_ref, links_ref, blocks):
    node = scal_ref[0]
    b0, b1, b2 = node % 2, node // 2 % 2, node // 4 % 2
    block = node // 8
    odd, has_left, has_right = block % 2, block > 0, block < blocks - 1

    def low_group(n):
        return jnp.where(b2 == 0, mine_ref[n], other_ref[n])

    def high_group(n):
        return jnp.where(b2 == 0, other_ref[n], mine_ref[n])

    crossed = (odd == 1) == (b0 == 0)

    def left(n):
        tile = jnp.where(crossed, first_ref[n], second_ref[n])
        return jnp.where(has_left, tile, jnp.zeros_like(tile))

    def right(n):
        tile = jnp.where(crossed, second_ref[n], first_ref[n])
        return jnp.where(has_right, tile, jnp.zeros_like(tile))

    def pick(j, options):
        tile = options[-1]
        for n in range(len(options) - 2, -1, -1):
            tile = jnp.where(j == n, options[n], tile)
        return tile

    ext0 = [left(2), low_group(0), low_group(1), high_group(0), high_group(1), right(2)]
    ext1 = [left(1), low_group(2), high_group(2), right(1)]
    j0, j1 = b2 * 2 + b1, b2
    around = [
        (pick(j0, ext0[:4]), pick(j0, ext0[2:])),
        (pick(j1, ext1[:2]), pick(j1, ext1[2:])),
        (left(0), right(0)),
    ]
    coupled = []
    for c, parity in enumerate((b0, b1, b2)):
        mid = links_ref[c, 1]
        none = jnp.zeros_like(mid)
        lo = jnp.concatenate([links_ref[c, 0], jnp.where(parity == 1, mid, none)], axis=0)
        hi = jnp.concatenate([jnp.where(parity == 0, mid, none), links_ref[c, 2]], axis=0)
        coupled.append(dot(around[c][0], lo) + dot(around[c][1], hi))
    h = coupled[1] + dot(coupled[2].astype(bf16), tree_ref[1, b1], NT)
    h = coupled[0] + dot(h.astype(bf16), tree_ref[0, b0], NT)
    return twice(h).astype(bf16)


def finish(near_ref, far_ref, basis_ref, transfer_ref, descent, coeffs_ref, out_ref):
    def coeffs(at):
        down = dot(descent, two_blocks(transfer_ref[:, at]), NT)
        coeffs_ref[:, at] = (far_ref[:, at] + down).astype(bf16)

    def result(at):
        out = near_ref[:, at] + dot(coeffs_ref[:, at], two_blocks(basis_ref[:, at]))
        out_ref[:, at] = out.astype(out_ref.dtype)

    count = near_ref.shape[1] // TILE
    by_tiles(count, coeffs)
    by_tiles(count, result)


def inner_kernel(
    scal_ref, near_ref, far_ref, basis_ref, transfer_ref,
    mine_ref, other_ref, first_ref, second_ref, tree_ref, links_ref,
    middle_ref, coeffs_ref, *, blocks,
):
    descent = descend(scal_ref, mine_ref, other_ref, first_ref, second_ref, tree_ref, links_ref, blocks)
    finish(near_ref, far_ref, basis_ref, transfer_ref, descent, coeffs_ref, middle_ref)


def next_kernel(scal_ref, tree_ref, rows_ref, basis_ref, transfer_ref, coords_ref, pay_ref):
    def coords(at):
        coords_ref[:, at] = dot(rows_ref[:, at], two_blocks(basis_ref[:, at]), NT).astype(bf16)

    by_tiles(rows_ref.shape[1] // TILE, coords)
    coarse_payload(node_sums(coords_ref, transfer_ref), tree_ref, scal_ref, pay_ref)


def outer_kernel(
    scal_ref, near_ref, far_ref, basis_ref, transfer_ref,
    mine_ref, other_ref, first_ref, second_ref, tree_ref, links_ref,
    samples_ref, work_ref, gram_ref, coeffs_ref, *, blocks,
):
    descent = descend(scal_ref, mine_ref, other_ref, first_ref, second_ref, tree_ref, links_ref, blocks)
    finish(near_ref, far_ref, basis_ref, transfer_ref, descent, coeffs_ref, samples_ref)
    low = low_half((LEAF, TILE))

    def step(g, total):
        for u in range(8):
            t = g * 8 + u
            both = jnp.concatenate([samples_ref[:, lanes(2 * t)], samples_ref[:, lanes(2 * t + 1)]], axis=0)
            both = dot3(both, both, NT)
            gram = jnp.where(low, both[:LEAF], both[LEAF:]) / TILE
            work_ref[t] = gram
            total = total + gram
        return total

    total = lax.fori_loop(0, work_ref.shape[0] // 8, step, jnp.zeros((LEAF, TILE), f32))
    total = total + swap_halves(total)
    half = LEAF // 2
    gram_ref[...] = jnp.where(low_half((half, TILE)), total[:half], total[half:])


def lane_take(tile, index):
    return jnp.take_along_axis(tile, index, axis=1, mode="promise_in_bounds")


def each(count, unroll, one):
    unroll = min(unroll, count)

    def step(g, carry):
        for u in range(unroll):
            one(g * unroll + u)
        return carry

    lax.fori_loop(0, count // unroll, step, 0)


def eliminate(work_ref, tee_ref, first=0, last=LEAF // 8):
    count = work_ref.shape[0]
    per = min(count, 4)
    groups = count // per
    sub = lax.broadcasted_iota(jnp.int32, (8, TILE), 0)
    lane = lax.broadcasted_iota(jnp.int32, (8, TILE), 1)
    col, half = lane % LEAF, lane // LEAF
    panels = LEAF // 8
    for kb in range(first, last):
        base = kb * 8
        rows = slice(base, base + 8)
        inside = (col >= base) & (col < base + 8)
        cols = []
        for g in range(groups):
            tiles = [work_ref[g * per + t, rows, :] for t in range(per)]
            packed = []
            for j in range(8):
                index = lane // 16 % 2 * LEAF + (base + j)
                value = lane_take(tiles[0], index)
                for t in range(1, per):
                    value = jnp.where(lane // 32 == t, lane_take(tiles[t], index), value)
                packed.append(value)
            cols.append(packed)
        tees = [[] for _ in range(groups)]
        for j in range(8):
            for c, tee in zip(cols, tees):
                inv = lax.rsqrt(c[j][j : j + 1, :])
                lower = c[j] * inv
                below = jnp.where(sub > j, lower, 0.0)
                for n in range(j + 1, 8):
                    c[n] = c[n] - lower * lower[n : n + 1, :]
                for n in range(j):
                    row = tee[n][j : j + 1, :] * inv
                    tee[n] = jnp.where(sub == j, row, tee[n] - below * row)
                tee.append(jnp.where(sub == j, inv, -below * inv))
        for g in range(groups):
            for j in range(8):
                tee_ref[g * 8 + j] = tees[g][j]

        for tt in range(per):
            index = tt * 32 + half * 16
            for g in range(groups):
                t = g * per + tt
                panel = work_ref[t, rows, :]
                spread = [lane_take(tee_ref[g * 8 + j], index) for j in range(8)]
                done = spread[0] * panel[:1, :]
                for j in range(1, 8):
                    done = done + spread[j] * panel[j : j + 1, :]
                for j in range(8):
                    done = jnp.where((col == base + j) & (sub >= j), spread[j], done)
                work_ref[t, rows, :] = done
        if kb == panels - 1:
            break

        rest_rows = LEAF - base - 8

        def update(t):
            left = work_ref[t, rows, :]
            right = jnp.where(inside & (col > base + sub), 0.0, left)
            turned = stacked(left, (0, 0, 1)).T.astype(bf16)
            turned = jnp.concatenate([turned[base + 8 : LEAF], turned[LEAF + base + 8 :]], axis=0)
            both = dot(turned, stacked(right, (0, 1, 0)).astype(bf16))
            for ib in range(kb + 1, panels):
                at = slice(ib * 8, ib * 8 + 8)
                n = (ib - kb - 1) * 8
                rest = jnp.where(inside, 0.0, work_ref[t, at, :])
                work_ref[t, at, :] = rest - jnp.where(half == 0, both[n : n + 8], both[rest_rows + n : rest_rows + n + 8])

        each(count, 16, update)


def stacked(x, order):
    high = x.astype(bf16).astype(f32)
    pieces = (high, x - high)
    return jnp.concatenate([pieces[n] for n in order] + [jnp.zeros_like(x)], axis=0)


def parts(tile):
    row = lax.broadcasted_iota(jnp.int32, tile.shape, 0)
    col = lax.broadcasted_iota(jnp.int32, tile.shape, 1) % LEAF
    return row, col


def pair_kernel(before_ref, work_ref, tee_ref, *, first, last):
    work_ref[...] = before_ref[...]
    eliminate(work_ref, tee_ref, first, last)


def solve_kernel(work_ref, samples_ref, basis_ref):
    def solve(t):
        tile = work_ref[t]
        row, col = parts(tile)
        inverse = two_blocks(jnp.where(col <= row, tile, 0.0))
        one, two = lanes(2 * t), lanes(2 * t + 1)
        solved = dot3(inverse, jnp.concatenate([samples_ref[:, one], samples_ref[:, two]], axis=0))
        basis_ref[:, one] = solved[:LEAF]
        basis_ref[:, two] = solved[LEAF:]

    each(work_ref.shape[0], 8, solve)


def eliminate_few(load, save, count):
    shape = (count, 8, TILE)
    sub = lax.broadcasted_iota(jnp.int32, shape, 1)
    lane = lax.broadcasted_iota(jnp.int32, shape, 2)
    low = lane < LEAF
    col = lane % LEAF
    panels = LEAF // 8
    for kb in range(panels):
        panel = load(kb)
        cols = []
        for j in range(8):
            k = kb * 8 + j
            one = jnp.broadcast_to(panel[:, :, k : k + 1], shape)
            two = jnp.broadcast_to(panel[:, :, LEAF + k : LEAF + k + 1], shape)
            cols.append(jnp.where(low, one, two))
        rows = []
        for j in range(8):
            k = kb * 8 + j
            inv = lax.rsqrt(cols[j][:, j : j + 1, :])
            lower = cols[j] * inv
            for n in range(j + 1, 8):
                cols[n] = cols[n] - lower * lower[:, n : n + 1, :]
            row = jnp.where(col[:, :1] == k, inv, panel[:, j : j + 1, :] * inv)
            below = sub > j
            kept = jnp.where(below & (col == k), 0.0, panel)
            panel = jnp.where(sub == j, row, kept - jnp.where(below, lower, 0.0) * row)
            rows.append(row)
        save(kb, panel)
        if kb == panels - 1:
            break
        turned = jnp.swapaxes(panel, 1, 2)
        inside = (col >= kb * 8) & (col < kb * 8 + 8)
        for j in range(8):
            k = kb * 8 + j
            rows[j] = jnp.where((col[:, :1] > k) & (col[:, :1] < kb * 8 + 8), 0.0, rows[j])
        for ib in range(kb + 1, panels):
            rest = jnp.where(inside, 0.0, load(ib))
            for j in range(8):
                one = jnp.broadcast_to(turned[:, ib * 8 : ib * 8 + 8, j : j + 1], shape)
                two = jnp.broadcast_to(turned[:, LEAF + ib * 8 : LEAF + ib * 8 + 8, j : j + 1], shape)
                rest = rest - jnp.where(low, one, two) * rows[j]
            save(ib, rest)


def group_kernel(gram_ref, work_ref, out_ref, own_ref, *, scale):
    packed = gram_ref[...] / scale
    other = swap_halves(packed)
    low = low_half(packed.shape)
    own_ref[0] = jnp.concatenate([jnp.where(low, packed, other), jnp.where(low, other, packed)], axis=0)

    def load(b):
        return own_ref[:, b * 8 : b * 8 + 8, :]

    def save(b, value):
        own_ref[:, b * 8 : b * 8 + 8, :] = value

    eliminate_few(load, save, 1)
    tile = own_ref[0]
    row, col = parts(tile)
    inverse = jnp.where(col <= row, tile, 0.0)

    def solve(t):
        tile = work_ref[t]
        upper = jnp.where(col > row, tile, jnp.where(col == row, 1.0 / tile, 0.0))
        out_ref[:, lanes(t)] = dot3(inverse, two_blocks(upper), NT)

    each(work_ref.shape[0], 8, solve)


HBM = pl.BlockSpec(memory_space=pltpu.HBM)
VMEM = pl.BlockSpec(memory_space=pltpu.VMEM)
SMEM = pl.BlockSpec(memory_space=pltpu.SMEM)


def params(mib):
    return pltpu.CompilerParams(vmem_limit_bytes=mib * 2**20)


def elimination(count):
    return [
        pltpu.VMEM((max(count // 4, 1) * 8, 8, TILE), f32),
    ]


def struct(shape, dtype):
    return jax.ShapeDtypeStruct(shape, dtype)


def swap(x, mask):
    count = lax.axis_size(AXES)
    return lax.ppermute(x, AXES, [(i, i ^ mask) for i in range(count)])


def adjacent_rows(x):
    count = lax.axis_size(AXES)
    route = []
    for i in range(count):
        forward = (i // 8 % 2 == 0) == (i % 2 == 0)
        route.append((i, (i + 8 if forward else i - 8) % count))
    return lax.ppermute(x, AXES, route)


def node_halo(x):
    count = lax.axis_size(AXES)
    route = [(i, (i - 1 if i % 2 == 0 else i + 1) % count) for i in range(count)]
    far = lax.ppermute(x, AXES, route)
    near = swap(x, 1)
    return far, near


def leaf_table(index, node):
    leaves = index.shape[0]
    place = index - (node - 1) * leaves
    block = place // leaves
    block = jnp.where(node % 2 == 1, 2 - block, block)
    place = block * leaves + place % leaves
    slot = lax.broadcasted_iota(jnp.int32, index.shape, 1)
    return (((place + slot) % 2) * (3 * leaves // 2) + place // 2).reshape(-1)


def coarse_near(pay, node):
    low = low_half((LEAF, TILE))
    b0, b1 = node % 2, node // 2 % 2

    def halves(bit, mine, other):
        return jnp.where(low == (bit == 0), mine, other)

    other = swap(pay, 1)
    z0 = halves(b0, pay[0], other[0])
    stage = jnp.stack([z0, pay[1] + other[1], pay[2] + other[2]])
    other = swap(stage, 2)
    first = jnp.where(b1 == 0, stage[0], other[0])
    second = jnp.where(b1 == 0, other[0], stage[0])
    return jnp.stack([first, second, halves(b1, stage[1], other[1]), stage[2] + other[2]])


def far_payload(mine, other, node):
    low = low_half((LEAF, TILE))
    b2, odd = node // 4 % 2, node // 8 % 2
    top = jnp.where(low == (b2 == 0), mine[3], other[3])
    lo = jnp.where(b2 == 0, mine, other)
    hi = jnp.where(b2 == 0, other, mine)
    rightward = jnp.stack([top, hi[2], hi[1]])
    leftward = jnp.stack([top, lo[2], lo[0]])
    return jnp.where((odd == 0) == (node % 2 == 0), rightward, leftward)


def after(x, *values):
    return lax.optimization_barrier((x, *values))[0]


def local(
    probes,
    near_index,
    far_index,
    inner_near,
    inner_basis,
    inner_far,
    inner_transfer,
    inner_tree,
    inner_links,
    outer_near,
    outer_basis,
    outer_far,
    outer_transfer,
    outer_tree,
    outer_links,
):
    node = lax.axis_index(AXES)
    count = lax.axis_size(AXES)
    width = probes.shape[1]
    scal = node.reshape(1).astype(jnp.int32)
    near_table = leaf_table(near_index, node)
    far_table = leaf_table(far_index, node)

    def interact(index, rows, blocks, bases=(), streamed=False):
        scratch = [pltpu.VMEM((3 * width // LEAF, LEAF, TILE), bf16)]
        if streamed:
            scratch += [pltpu.VMEM(blocks.shape, bf16), pltpu.SemaphoreType.DMA((STEPS,))]
        return pl.pallas_call(
            lambda *refs: interact_kernel(*refs, streamed=streamed),
            in_specs=[SMEM] + [VMEM] * (3 + len(bases)) + [HBM if streamed else VMEM],
            out_specs=VMEM,
            out_shape=struct((LEAF, width), f32),
            scratch_shapes=scratch,
            compiler_params=params(56 if streamed else 6),
            name="interact",
        )(index, *rows, *bases, blocks)

    def next_step(*args, **kwargs):
        return pl.pallas_call(*args, **kwargs)

    row = struct((LEAF, width), bf16)
    payload = struct((3, LEAF, TILE), bf16)
    pairs = width // TILE

    rows_b, rows_a = node_halo(probes)
    coords, pay, rows, basis, transfer = pl.pallas_call(
        coords_kernel,
        in_specs=[SMEM, HBM, HBM, HBM, HBM],
        out_specs=(VMEM,) * 5,
        out_shape=(row, payload, row, row, row),
        scratch_shapes=[
            pltpu.VMEM(inner_tree.shape, bf16),
            pltpu.SemaphoreType.DMA((3, STEPS // 2)),
            pltpu.SemaphoreType.DMA,
        ],
        compiler_params=params(52),
        name="coords",
    )(scal, inner_tree, probes, inner_basis, inner_transfer)
    mine = coarse_near(pay, node)
    mine, near_table, far_table = lax.optimization_barrier((mine, near_table, far_table))
    other = swap(mine, 6)
    coords_b, coords_a = node_halo(after(coords, mine))
    near_part = interact(near_table, (rows_b, after(rows, mine), rows_a), inner_near, streamed=STREAM[0])
    other, near_part = lax.optimization_barrier((other, near_part))
    one = adjacent_rows(far_payload(mine, other, node))
    basis_b, basis_a = node_halo(after(outer_basis, near_part))
    far_part = interact(far_table, (coords_b, coords, coords_a), inner_far, streamed=STREAM[1])
    one, far_part = lax.optimization_barrier((one, far_part))
    two = swap(one, 1)
    middle = pl.pallas_call(
        lambda *refs: inner_kernel(*refs, blocks=count // 8),
        in_specs=[SMEM] + [VMEM] * 10,
        out_specs=VMEM,
        out_shape=row,
        scratch_shapes=[pltpu.VMEM((LEAF, width), bf16)],
        compiler_params=params(6),
        name="inner",
    )(scal, near_part, far_part, basis, transfer, mine, other, one, two, inner_tree, inner_links)
    middle_b, middle_a = node_halo(middle)
    coords, pay = next_step(
        next_kernel,
        in_specs=[SMEM] + [VMEM] * 4,
        out_specs=(VMEM, VMEM),
        out_shape=(row, payload),
        compiler_params=params(6),
        name="next",
    )(scal, outer_tree, middle, outer_basis, outer_transfer)
    mine = coarse_near(pay, node)
    other = swap(mine, 6)
    near_part = interact(near_table, (middle_b, after(middle, mine), middle_a), outer_near)
    other, near_part = lax.optimization_barrier((other, near_part))
    one = adjacent_rows(far_payload(mine, other, node))
    far_part = interact(far_table, (middle_b, coords, middle_a), outer_far, (basis_b, basis_a))
    one, far_part = lax.optimization_barrier((one, far_part))
    two = swap(one, 1)
    samples, grams, gram = pl.pallas_call(
        lambda *refs: outer_kernel(*refs, blocks=count // 8),
        in_specs=[SMEM] + [VMEM] * 10,
        out_specs=(VMEM,) * 3,
        out_shape=(
            struct((LEAF, width), f32),
            struct((pairs // 2, LEAF, TILE), f32),
            struct((LEAF // 2, TILE), f32),
        ),
        scratch_shapes=[pltpu.VMEM((LEAF, width), bf16)],
        compiler_params=params(6),
        name="outer",
    )(scal, near_part, far_part, outer_basis, outer_transfer, mine, other, one, two, outer_tree, outer_links)

    def piece(n, work):
        return pl.pallas_call(
            lambda *refs: pair_kernel(*refs, first=2 * n, last=2 * n + 2),
            in_specs=[VMEM],
            out_specs=VMEM,
            out_shape=struct(work.shape, f32),
            scratch_shapes=elimination(pairs // 2),
            input_output_aliases={0: 0},
            compiler_params=params(6),
            name="pairs",
        )(work)

    work = grams
    for n, mask in enumerate((1, 2, 6, 8)):
        other = swap(gram, mask)
        work = piece(n, work)
        gram, work = lax.optimization_barrier((gram + other, work))
    other = swap(gram, 24)
    pair_basis = pl.pallas_call(
        solve_kernel,
        in_specs=[VMEM, VMEM],
        out_specs=VMEM,
        out_shape=struct((LEAF, width), f32),
        compiler_params=params(6),
        name="solve",
    )(work, samples)
    gram = gram + other
    scale = pairs * lax.axis_size("leaf")
    group_basis = pl.pallas_call(
        lambda *refs: group_kernel(*refs, scale=scale),
        in_specs=[VMEM, VMEM],
        out_specs=VMEM,
        out_shape=struct((LEAF, pairs * LEAF), f32),
        scratch_shapes=[pltpu.VMEM((1, LEAF, TILE), f32)],
        compiler_params=params(6),
        name="group",
    )(gram, work)
    return (pair_basis, group_basis)


def solution(mesh):
    flat = P(None, AXES)
    index = P(AXES, None)
    blocks = P(None, None, AXES)
    tree = P(None, None, None, AXES)
    factor = (blocks, flat, blocks, flat, tree, tree)
    return jax.shard_map(
        local,
        mesh=mesh,
        in_specs=(flat, index, index) + factor + factor,
        out_specs=(flat, flat),
        check_vma=False,
    )
```
